512 devices in a mesh: freq: 128 (over y, z, core), rows: 4 (over x).
Axes of the slice: x: 4, y: 8, z: 8, core: 2. Of those that a mesh axis runs over, the one named last changes fastest.
Arguments:
- wavefield: bfloat16 [10240, 32, 1024], P('freq', 'rows'), may hold values from -6 to 6
- u_factors: bfloat16 [2, 256, 4, 256, 512], P(None, 'freq', 'rows'), may hold values from -0.25 to 0.25
- v_factors: bfloat16 [2, 256, 4, 512, 256], P(None, 'freq', 'rows'), may hold values from -0.375 to 0.375
- tile_ranks: int32 [256, 4, 40], P('freq', 'rows'), may hold values from 1 to 64, as said below
- tile_offsets: int32 [256, 4, 40], P('freq', 'rows'), may hold values from 0 to 511, as said below
Outputs:
- convolved: bfloat16 [1024, 32, 1024], P(('rows', 'freq'))
The draws below stay inside these ranges and needn't reach their ends.
Inputs may be any that keep to these rules, and one draw needn't show every extreme that they name: tile_ranks[k, i, j] is the rank of tile (i, j) of frequency k; the ranks of one tile row sum to at most 512, exactly 512 on some row of every draw, and every tile row has a tile of rank 64. tile_offsets[k, i, j] is the sum of tile_ranks[k, i, j2] over j2 < j.
All inputs are finite; a program needn't handle non-finite values.
Results may differ from the reference program's by a relative error of at most 0.0072.
Values may be sent and summed in bfloat16 or wider, within the bound.
A program may use at most 128 MiB of HBM per device.

```python
import math
import jax
import jax.numpy as jnp
from jax import lax

RECEIVERS = 10240
SAMPLES = 1024
TILE = 256
RANK_MAX = 64
SLOTS = 512
SOURCES = 32
FREQS = 256
TILE_ROWS = 4
TILE_COLS = 40


def rank_tables(key):
    base_key = jax.random.fold_in(key, 4242)
    key_weight, key_target, key_chosen, key_peak = jax.random.split(base_key, 4)
    weight = jax.random.randint(key_weight, (FREQS, TILE_ROWS, TILE_COLS), 1, 65)
    weight = weight * weight // 64 + 1
    target = SLOTS // 2 + jax.random.randint(key_target, (FREQS, TILE_ROWS), 0, SLOTS - SLOTS // 2 + 1)
    chosen = jax.random.randint(key_chosen, (), 0, FREQS * TILE_ROWS)
    row_number = jnp.arange(FREQS * TILE_ROWS, dtype=jnp.int32).reshape(FREQS, TILE_ROWS)
    target = jnp.where(row_number == chosen, SLOTS, target)
    peak_tile = jax.random.randint(key_peak, (FREQS, TILE_ROWS, 1), 0, TILE_COLS)
    is_peak = jnp.arange(TILE_COLS, dtype=jnp.int32)[None, None, :] == peak_tile
    spare_slots = target - (TILE_COLS - 1) - RANK_MAX
    others = jnp.where(is_peak, 0, weight)
    weight_sum = jnp.sum(others, axis=2)
    base_rank = jnp.minimum(1 + others * spare_slots[:, :, None] // weight_sum[:, :, None], RANK_MAX)
    rank_table = jnp.where(is_peak, RANK_MAX, base_rank)
    deficit = target - jnp.sum(rank_table, axis=2)
    headroom = jnp.where(is_peak, 0, RANK_MAX - rank_table)
    before = jnp.cumsum(headroom, axis=2) - headroom
    rank_table = rank_table + jnp.clip(deficit[:, :, None] - before, 0, headroom)
    starts = jnp.cumsum(rank_table, axis=2) - rank_table
    return (rank_table.astype(jnp.int32), starts.astype(jnp.int32))


def draw_tile_ranks(key, part):
    return rank_tables(key)[0]


def draw_tile_offsets(key, part):
    return rank_tables(key)[1]


def level_of(rng, shape, cuts, least, top_value):
    def one(dim, parts):
        steps = jax.random.uniform(jax.random.fold_in(jax.random.fold_in(rng, 6), dim), (parts,), jnp.float32, least / len(cuts), top_value / len(cuts))
        return jnp.repeat(jnp.exp(steps), shape[dim] // parts).reshape((-1,) + (1,) * (len(shape) - dim - 1))

    gain = one(*cuts[0])
    for cut in cuts[1:]:
        gain = gain * one(*cut)
    return gain


def gaussian(stream_key, shape, spread, most, shards=(), kind=jnp.bfloat16):
    entries = jax.random.normal(stream_key, shape, jnp.float32) * spread
    if len(shards) > 0:
        entries = level_of(stream_key, shape, shards, -0.22, 0.18) * entries
    return jnp.clip(entries, min=-most, max=most).astype(kind)


def setup_inputs(seed: int = 0) -> dict:
    seeds = jax.random.split(jax.random.key(seed), 6)
    return {
        "wavefield": gaussian(seeds[0], (RECEIVERS, SOURCES, SAMPLES), 1.0, 6.0, ((0, 128), (1, 4))),
        "u_factors": gaussian(seeds[1], (2, FREQS, TILE_ROWS, TILE, SLOTS), SLOTS ** -0.5, 0.25, ((1, 128), (2, 4))),
        "v_factors": gaussian(seeds[2], (2, FREQS, TILE_ROWS, SLOTS, TILE), TILE ** -0.5, 0.375, ((1, 128), (2, 4))),
        "tile_ranks": draw_tile_ranks(jax.random.fold_in(seeds[5], 71), 0),
        "tile_offsets": draw_tile_offsets(jax.random.fold_in(seeds[5], 71), 0),
    }


def spectral_tables(freq_count, sample_count):
    freq_bins = jnp.arange(freq_count, dtype=jnp.int32) + 1
    sample_index = jnp.arange(sample_count, dtype=jnp.int32)
    phase_int = freq_bins[:, None] * sample_index[None, :] % sample_count
    angles = phase_int.astype(jnp.float32) * (2.0 * math.pi / sample_count)
    cosine = jnp.cos(angles)
    minus_sine = -jnp.sin(angles)
    stacked = jnp.stack([cosine, minus_sine], axis=1)
    forward = (stacked / math.sqrt(sample_count)).astype(jnp.bfloat16)
    inverse = (stacked / math.sqrt(freq_count)).astype(jnp.bfloat16)
    return (forward, inverse)

def tile_windows(v_row, u_row, starts, rank_max):
    columns = starts.shape[0]
    slot_index = (starts[:, None] + jnp.arange(rank_max, dtype=jnp.int32)[None, :]).reshape(-1)
    v_padded = jnp.pad(v_row, ((0, 0), (0, rank_max), (0, 0)))
    u_padded = jnp.pad(u_row, ((0, 0), (0, 0), (0, rank_max)))
    v_win = jnp.take(v_padded, slot_index, axis=1).reshape(2, columns, rank_max, v_row.shape[2])
    u_win = jnp.take(u_padded, slot_index, axis=2).reshape(2, u_row.shape[1], columns, rank_max)
    return (v_win, u_win)

def tile_row_product(u_row, v_row, counts, starts, spectra):
    v_win, u_win = tile_windows(v_row, u_row, starts, RANK_MAX)
    quadrants = jnp.einsum('ajmr,jbrs->abjms', v_win.astype(jnp.float32), spectra.astype(jnp.float32))
    real_part = quadrants[0, 0] - quadrants[1, 1]
    imag_part = quadrants[0, 1] + quadrants[1, 0]
    rank_mask = jnp.arange(RANK_MAX, dtype=jnp.int32)[None, :] < counts[:, None]
    coeffs = jnp.where(rank_mask[None, :, :, None], jnp.stack([real_part, imag_part]), 0.0).astype(jnp.bfloat16)
    products = jnp.einsum('arjm,cjms->acrs', u_win.astype(jnp.float32), coeffs.astype(jnp.float32))
    return jnp.stack([products[0, 0] - products[1, 1], products[0, 1] + products[1, 0]]).astype(jnp.bfloat16)

def reference(wavefield, u_factors, v_factors, tile_ranks, tile_offsets):
    receivers, sources, samples = wavefield.shape
    freqs = u_factors.shape[1]
    tile_rows = u_factors.shape[2]
    tile_size = u_factors.shape[3]
    columns = receivers // tile_size
    forward, inverse = spectral_tables(freqs, samples)
    blocks = wavefield.reshape(columns, tile_size, sources, samples)

    def transform(block):
        return jnp.einsum('kct,rst->kcrs', forward.astype(jnp.float32), block.astype(jnp.float32)).astype(jnp.bfloat16)
    spectrum = jnp.moveaxis(lax.map(transform, blocks), 1, 0)

    def one_band(items):
        spectra, u_band, v_band, counts, starts = items
        rows_out = [tile_row_product(u_band[:, tile_row], v_band[:, tile_row], counts[tile_row], starts[tile_row], spectra) for tile_row in range(tile_rows)]
        return jnp.stack(rows_out, axis=1)
    bands = lax.map(one_band, (spectrum, jnp.moveaxis(u_factors, 1, 0), jnp.moveaxis(v_factors, 1, 0), tile_ranks, tile_offsets))
    flat_bands = bands.reshape(freqs, 2, tile_rows * tile_size * sources)
    series = jnp.einsum('kcq,kct->qt', flat_bands.astype(jnp.float32), inverse.astype(jnp.float32))
    return series.reshape(tile_rows * tile_size, sources, samples).astype(jnp.bfloat16)
```

```python
import functools
import math

import jax
import jax.numpy as jnp
from jax import lax
from jax.experimental import pallas as pl
from jax.experimental.pallas import tpu as pltpu
from jax.sharding import Mesh
from jax.sharding import PartitionSpec as P

FREQ = ("freq_0", "freq_1", "freq_2")
ROWS_FREQ = ("rows", "freq_0", "freq_1", "freq_2")
BF = jnp.bfloat16
F32 = jnp.float32


def tables(freqs, samples):
    row = jnp.arange(2 * freqs, dtype=jnp.int32)
    g, y, kk, c = row // 32, (row // 4) % 8, (row // 2) % 2, row % 2
    k = 2 * (y * 16 + g) + kk
    t = jnp.arange(samples, dtype=jnp.int32)
    phase = ((k + 1)[:, None] * t[None, :]) % samples
    angle = phase.astype(F32) * (2.0 * math.pi / samples)
    value = jnp.where(c[:, None] == 0, jnp.cos(angle), -jnp.sin(angle))
    forward = (value / math.sqrt(samples)).astype(BF)
    inverse = (value / math.sqrt(freqs)).astype(BF)
    inverse = inverse.reshape(128, 4, samples)
    inverse = jnp.transpose(inverse, (1, 0, 2)).reshape(2 * freqs, samples)
    return forward, inverse


def dft_kernel(w_ref, f_ref, out_ref, o_ref):
    for gb in range(4):
        o_ref[gb] = lax.dot_general(
            w_ref[...], f_ref[pl.ds(gb * 128, 128)], (((1,), (1,)), ((), ())), preferred_element_type=F32
        )
    slot = lax.broadcasted_iota(jnp.int32, (16, 128), 1) // 16
    for chunk in range(5):
        for gb in range(4):
            turned = []
            for s in range(8):
                x = o_ref[gb, pl.ds(chunk * 128 + s, 16, stride=8), :]
                turned.append(pltpu.roll(x, 16 * s, axis=1) if s else x)
            for b in range(8):
                acc = turned[(-b) % 8]
                for p in range(1, 8):
                    acc = jnp.where(slot == p, turned[(p - b) % 8], acc)
                out_ref[gb * 4 + b // 2, pl.ds(chunk * 16, 16), pl.ds((b % 2) * 128, 128)] = acc.astype(BF)


def lane_permutation(h, gamma):
    col = lax.broadcasted_iota(jnp.int32, (512, 512), 1)
    row = lax.broadcasted_iota(jnp.int32, (512, 512), 0)
    y_lo, kk, j, c, s = col // 128, (col // 64) % 2, (col // 16) % 4, (col // 8) % 2, col % 8
    p = (s + 2 * gamma + h) % 8
    source = j * 128 + p * 16 + y_lo * 4 + kk * 2 + c
    return jnp.where(row == source, 1.0, 0.0).astype(BF)


def fold_kernel(a_ref, out_ref):
    gamma = (lax.axis_index("freq_1") * 2 + lax.axis_index("freq_2")) % 4
    for h in range(2):
        lanes = pl.ds(h * 128, 128)
        main = jnp.concatenate([a_ref[pl.ds(j * 256, 256), lanes] for j in range(4)], axis=1)
        last = jnp.concatenate([a_ref[pl.ds(1024 + q * 64, 64), lanes] for q in range(4)], axis=1)
        both = jnp.concatenate([main, last], axis=0)
        moved = jnp.dot(both, lane_permutation(h, gamma), preferred_element_type=F32).astype(BF)
        for y in range(4):
            out_ref[h * 4 + y] = moved[:, y * 128 : (y + 1) * 128]


def half_lanes(a, b, kk):
    low = lax.broadcasted_iota(jnp.int32, a.shape, 1) < 64
    if kk == 0:
        return jnp.where(low, a, pltpu.roll(b, 64, axis=1))
    return jnp.where(low, pltpu.roll(a, 64, axis=1), b)


def swapped(b, width):
    lane = lax.broadcasted_iota(jnp.int32, b.shape, 1)
    real = (lane // width) % 2 == 0
    size = b.shape[1]
    return jnp.where(real, -pltpu.roll(b, size - width, axis=1), pltpu.roll(b, width, axis=1))


def tile_kernel(g_ref, v_ref, u_ref, rank_ref, start_ref, out_ref, fifth_ref, acc_ref):
    lane1 = lax.broadcasted_iota(jnp.int32, (512, 128), 1)
    col = lax.broadcasted_iota(jnp.int32, (512, 512), 1)
    row = lax.broadcasted_iota(jnp.int32, (512, 512), 0)
    q, kk_, x_, cs = col // 128, (col // 64) % 2, (col // 16) % 4, col % 16
    perm = jnp.where(row == x_ * 128 + kk_ * 64 + q * 16 + cs, 1.0, 0.0).astype(BF)
    for y in range(8):
        lhs = jnp.concatenate([g_ref[x, y, pl.ds(256, 64), :] for x in range(4)], axis=1)
        moved = jnp.dot(lhs, perm, preferred_element_type=F32)
        for b in range(4):
            fifth_ref[y, pl.ds(b * 64, 64), :] = moved[:, b * 128 : (b + 1) * 128]
    coeffs = []
    tgt = lax.broadcasted_iota(jnp.int32, (256, 128), 1)
    src = lax.broadcasted_iota(jnp.int32, (256, 128), 0)
    for kk in range(2):
        starts = start_ref[kk]
        ranks = rank_ref[kk]
        total = jnp.max(starts + ranks, axis=1, keepdims=True)
        slot40 = lax.broadcasted_iota(jnp.int32, (512, 40), 0)
        begun = jnp.where(starts <= slot40, 1.0, 0.0) + jnp.where(total <= slot40, 64.0, 0.0)
        owner = jnp.sum(begun, axis=1, keepdims=True).astype(jnp.int32) - 1
        v = v_ref[:, kk].reshape(1024, 256)
        acc_ref[...] = jnp.zeros_like(acc_ref)
        for part in range(2):
            if part == 0:
                place = owner - (lane1 // 16) % 4
            else:
                place = owner - 5 * (lane1 // 64)
            for y in range(8 if part == 0 else 2):
                if part == 0:
                    pairs = [(g_ref[2 * m, y, pl.ds(0, 256), :].astype(F32),
                              g_ref[2 * m + 1, y, pl.ds(0, 256), :].astype(F32)) for m in range(2)]
                else:
                    pairs = [(fifth_ref[4 * y + 2 * m], fifth_ref[4 * y + 2 * m + 1]) for m in range(2)]
                rhs = jnp.concatenate([half_lanes(a, b, kk) for a, b in pairs], axis=1).astype(BF)
                prod = jnp.dot(v, rhs, preferred_element_type=F32)
                for m in range(2):
                    lanes = pl.ds(m * 128, 128)
                    if part == 0:
                        hit = place == 5 * y
                    else:
                        hit = place == 5 * (4 * y + 2 * m) + 4
                    for ab in range(2):
                        rows = pl.ds(ab * 512, 512)
                        acc_ref[part, rows, lanes] = jnp.where(
                            hit, prod[ab * 512 : (ab + 1) * 512, m * 128 : (m + 1) * 128], acc_ref[part, rows, lanes]
                        )
        total_c = jnp.zeros((512, 128), F32)
        for part in range(2):
            if part == 0:
                xs, c, s = src // 64, (src // 8) % 2, src % 8
            else:
                xs, c, s = (src // 16) % 4, (src // 8) % 2, src % 8
            join = jnp.where(tgt == kk * 64 + c * 32 + xs * 8 + s, 1.0, 0.0).astype(BF)
            for m in range(2):
                lanes = pl.ds(m * 128, 128)
                value = acc_ref[part, pl.ds(0, 512), lanes] + swapped(acc_ref[part, pl.ds(512, 512), lanes], 8)
                total_c = total_c + jnp.dot(
                    value.astype(BF), join[m * 128 : (m + 1) * 128], preferred_element_type=F32
                )
        coeffs.append(total_c.astype(BF))
    e = jnp.zeros((512, 128), F32)
    for kk in range(2):
        e = e + jnp.dot(u_ref[:, kk].reshape(512, 512), coeffs[kk], preferred_element_type=F32)
    out_ref[...] = (e[:256] + swapped(e[256:], 32)).astype(BF)


VM = pl.BlockSpec(memory_space=pltpu.VMEM)
PARAMS = pltpu.CompilerParams(vmem_limit_bytes=60 * 1024 * 1024)


def per_device(wavefield, u_factors, v_factors, tile_ranks, tile_offsets):
    forward, inverse = tables(256, 1024)
    chunks = pl.pallas_call(
        dft_kernel,
        out_shape=jax.ShapeDtypeStruct((16, 80, 256), BF),
        in_specs=[VM, VM],
        out_specs=VM,
        scratch_shapes=[pltpu.VMEM((4, 640, 128), F32)],
        compiler_params=PARAMS,
    )(wavefield.reshape(640, 1024), forward)
    got = lax.all_to_all(chunks, ("freq_1", "freq_2"), 0, 0, tiled=True)
    folded = pl.pallas_call(
        fold_kernel,
        out_shape=jax.ShapeDtypeStruct((8, 320, 128), BF),
        in_specs=[VM],
        out_specs=VM,
        compiler_params=PARAMS,
    )(got.reshape(1280, 256))
    mine = lax.all_to_all(folded, "freq_0", 0, 0, tiled=True)
    copies = jnp.broadcast_to(mine, (4, *mine.shape))
    gathered = lax.all_to_all(copies, "rows", 0, 0, tiled=True)
    bands = pl.pallas_call(
        tile_kernel,
        out_shape=jax.ShapeDtypeStruct((256, 128), BF),
        in_specs=[VM] * 5,
        out_specs=VM,
        scratch_shapes=[pltpu.VMEM((8, 256, 128), F32), pltpu.VMEM((2, 1024, 256), F32)],
        compiler_params=PARAMS,
    )(gathered, v_factors[:, :, 0], u_factors[:, :, 0], tile_ranks, tile_offsets)
    first = lax.all_to_all(bands.reshape(8, 32, 128), "freq_0", 0, 0, tiled=True)
    first = jnp.transpose(first.reshape(8, 16, 2, 128), (1, 0, 2, 3))
    second = lax.all_to_all(first, ("freq_1", "freq_2"), 0, 0, tiled=True)
    lhs = jnp.transpose(second.reshape(128, 2, 4, 32), (1, 3, 2, 0)).reshape(64, 512)
    series = jnp.dot(lhs, inverse, preferred_element_type=F32)
    return series.astype(BF).reshape(2, 32, 1024)


def solution(mesh):
    torus = Mesh(
        mesh.devices.reshape(8, 8, 2, mesh.shape["rows"]), ("freq_0", "freq_1", "freq_2", "rows")
    )
    return jax.shard_map(
        per_device,
        mesh=torus,
        in_specs=(
            P(FREQ, "rows", None),
            P(None, FREQ, "rows", None, None),
            P(None, FREQ, "rows", None, None),
            P(FREQ, "rows", None),
            P(FREQ, "rows", None),
        ),
        out_specs=P(ROWS_FREQ, None, None),
        check_vma=False,
    )
```

```python
import math

import jax
import jax.numpy as jnp
import numpy as np
from jax import lax
from jax.experimental import pallas as pl
from jax.experimental.pallas import tpu as pltpu
from jax.sharding import Mesh
from jax.sharding import PartitionSpec as P

FREQ = ("freq_0", "freq_1", "freq_2")
ROWS_FREQ = ("rows", "freq_0", "freq_1", "freq_2")
BF = jnp.bfloat16
F32 = jnp.float32
MESH = pl.DeviceIdType.MESH

_z = 0.125 * (1.0 - np.cos(np.pi * (np.arange(64) + 0.5) / 64))
COS = [float(a) for a in np.polynomial.polynomial.polyfit(_z, np.cos(2 * np.pi * np.sqrt(_z)), 9)]

STEPS = [(0, 1)] + [(d, c) for n in (1, 2, 3) for d in (n, 8 - n) for c in (0, 1)] + [(4, 0), (4, 1)]
YSTEPS = (1, 7, 2, 6, 3, 5, 4)


def cosine(m):
    x = jnp.where(m >= 512, m - 1024, m).astype(F32) * (1.0 / 1024.0)
    z = x * x
    value = jnp.full(m.shape, COS[-1], F32)
    for a in COS[-2::-1]:
        value = value * z + a
    return value


def build_table(f_ref, kk):
    for part in range(4):
        row = lax.broadcasted_iota(jnp.int32, (64, 128), 0) + part * 64
        lane = lax.broadcasted_iota(jnp.int32, (64, 128), 1)
        k1 = (row // 2) * 2 + (kk + 1)
        m = (k1 * lane + (row % 2) * 256) & 1023
        co, si = cosine(m), cosine((m + 768) & 1023)
        turn = (k1 * 128) & 1023
        ct, st = cosine(turn), cosine((turn + 768) & 1023)
        for b in range(8):
            f_ref[kk, pl.ds(part * 64, 64), pl.ds(b * 128, 128)] = (co * (1.0 / 32.0)).astype(BF)
            if b < 7:
                co, si = co * ct - si * st, si * ct + co * st


def one_hot(shape, source):
    row = lax.broadcasted_iota(jnp.int32, shape, 0)
    return jnp.where(row == source, 1.0, 0.0).astype(BF)


def swapped(b, width):
    lane = lax.broadcasted_iota(jnp.int32, b.shape, 1)
    real = (lane // width) % 2 == 0
    return jnp.where(real, -pltpu.roll(b, b.shape[1] - width, axis=1), pltpu.roll(b, width, axis=1))


def kernel(
    w_hbm, v_hbm, u_hbm, rank_ref, start_ref, out_ref,
    w, v, u, f, o, s1, r1, perm, p2, g, place, acc, table, bb, ry, pz, rz,
    load_sem, s1s, r1s, p2s, p2r, xs, xm, xp, x2, xs2, f1s, f1r, f2s, f2r,
):
    y = lax.axis_index("freq_0")
    z = lax.axis_index("freq_1")
    core = lax.axis_index("freq_2")
    x = lax.axis_index("rows")
    me_g = z * 2 + core

    loads = [pltpu.make_async_copy(w_hbm, w, load_sem.at[0])]
    for kk in range(2):
        loads.append(pltpu.make_async_copy(v_hbm.at[:, kk], v.at[kk], load_sem.at[1 + kk]))
        loads.append(pltpu.make_async_copy(u_hbm.at[:, kk], u.at[kk], load_sem.at[3 + kk]))
    for load in loads:
        load.start()

    def y_peer(d):
        return {"freq_0": (y + d) % 8}

    def g_peer(d):
        return {"freq_1": (z + d[0]) % 8, "freq_2": (core + d[1]) % 2}

    def g_to(d):
        return ((z + d[0]) % 8) * 2 + (core + d[1]) % 2

    def g_from(d):
        return ((z + 8 - d[0]) % 8) * 2 + (core + 2 - d[1]) % 2

    x_up, x_down = (x + 1) % 4, (x + 3) % 4

    barrier = pltpu.get_barrier_semaphore()
    for d in YSTEPS:
        pl.semaphore_signal(barrier, inc=1, device_id=y_peer(d), device_id_type=MESH)
    for d in STEPS:
        pl.semaphore_signal(barrier, inc=1, device_id=g_peer(d), device_id_type=MESH)
    for peer in (x_up, x_down):
        pl.semaphore_signal(barrier, inc=1, device_id={"rows": peer}, device_id_type=MESH)

    def send(src, dst, ssem, rsem, peer):
        return pltpu.make_async_remote_copy(
            src_ref=src, dst_ref=dst, send_sem=ssem, recv_sem=rsem, device_id=peer, device_id_type=MESH
        )

    def y_copy(kk, i):
        d = YSTEPS[i]
        return send(s1.at[kk, (y + d) % 8], r1.at[kk, y], s1s.at[kk, i], r1s.at[kk, i], y_peer(d))

    def g_copy(kk, i):
        d = STEPS[i]
        rows = pl.ds(me_g * 80, 80)
        return send(p2.at[kk, g_to(d)], g.at[x, kk, rows], p2s.at[kk, i], p2r.at[kk, i], g_peer(d))

    def block(kk, i, owner):
        gs = me_g if i == 0 else g_from(STEPS[i - 1])
        return g.at[owner, kk, pl.ds(gs * 80, 80)]

    def x_copy(kk, i, up):
        ref = block(kk, i, x)
        if up:
            return send(ref, ref, xs.at[kk, 0], xm.at[kk, i], {"rows": x_up})
        return send(ref, ref, xs.at[kk, 1], xp.at[kk, i], {"rows": x_down})

    def x_relay(kk, i):
        if i % 2 == 0:
            ref = block(kk, i, x_down)
            return send(ref, ref, xs2.at[kk, 0], x2.at[kk], {"rows": x_up})
        ref = block(kk, i, x_up)
        return send(ref, ref, xs2.at[kk, 1], x2.at[kk], {"rows": x_down})

    def dft(kk):
        for half in range(2):
            o[half] = lax.dot_general(
                w[...], f[kk, pl.ds(half * 128, 128)], (((1,), (1,)), ((), ())), preferred_element_type=F32
            )
        slot = lax.broadcasted_iota(jnp.int32, (16, 128), 1) // 16

        def place_rows(chunk, carry):
            for half in range(2):
                turned = []
                for s in range(8):
                    t = o[half, pl.ds(chunk * 128 + s, 16, stride=8), :]
                    turned.append(pltpu.roll(t, 16 * s, axis=1) if s else t)
                for b in range(8):
                    value = turned[(-b) % 8]
                    for q in range(1, 8):
                        value = jnp.where(slot == q, turned[(q - b) % 8], value)
                    rows = pl.ds(pl.multiple_of(chunk * 16, 16), 16)
                    s1[kk, half * 4 + b // 2, rows, pl.ds((b % 2) * 128, 128)] = value.astype(BF)
            return carry

        lax.fori_loop(0, 5, place_rows, 0)

    def y_send(kk):
        for i in range(7):
            y_copy(kk, i).start()
        r1[kk, y] = s1[kk, y]

    def g_send(kk):
        for i in range(7):
            y_copy(kk, i).wait_recv()
        lhs = jnp.concatenate(
            [
                jnp.concatenate([r1[kk, a, :, pl.ds(h * 128, 128)] for a in range(8)], axis=1)
                for h in range(2)
            ],
            axis=0,
        )
        for b in range(8):
            moved = jnp.dot(lhs, perm[:, pl.ds(b * 128, 128)], preferred_element_type=F32).astype(BF)
            p2[kk, b] = moved[:80]
            p2[kk, 8 + b] = moved[80:]
        for i in range(15):
            g_copy(kk, i).start()
        g[x, kk, pl.ds(pl.multiple_of(me_g * 80, 16), 80)] = p2[kk, me_g]

    def forward(kk, i):
        if i > 0:
            g_copy(kk, i - 1).wait_recv()
        x_copy(kk, i, True).start()
        x_copy(kk, i, False).start()

    def relay(kk, i):
        x_copy(kk, i, True).wait_recv()
        x_copy(kk, i, False).wait_recv()
        x_relay(kk, i).start()

    def whole(kk, owner, ssem, rsem, rows=1280):
        ref = g.at[owner, kk, pl.ds(0, rows)]
        return send(ref, ref, ssem, rsem, {"rows": x_up})

    def settle(kk):
        whole(kk, x, xs.at[kk, 0], x2.at[kk]).wait_recv()

    def products(kk, jj):
        for half in range(2):
            rows = pl.ds(jj * 256, 256)
            rhs = jnp.concatenate([g[2 * half, kk, rows, :], g[2 * half + 1, kk, rows, :]], axis=1)
            prod = jnp.dot(v[kk].reshape(1024, 256), rhs, preferred_element_type=F32)
            for m in range(2):
                hit = place[kk] == jj
                lanes = pl.ds((2 * half + m) * 128, 128)
                for ab in range(2):
                    old = acc[pl.ds(ab * 512, 512), lanes] if jj else 0.0
                    new = prod[ab * 512 : (ab + 1) * 512, m * 128 : (m + 1) * 128]
                    acc[pl.ds(ab * 512, 512), lanes] = jnp.where(hit, new, old)

    def coefficients(kk):
        turn = (y % 4) * 2 + z // 4
        row = lax.broadcasted_iota(jnp.int32, (128, 128), 0)
        col = lax.broadcasted_iota(jnp.int32, (128, 128), 1)
        c, s = (row // 8) % 2, (row % 8 + 8 - turn) % 8
        total = jnp.zeros((512, 128), F32)
        for b in range(4):
            lanes = pl.ds(b * 128, 128)
            value = acc[pl.ds(0, 512), lanes] + swapped(acc[pl.ds(512, 512), lanes], 8)
            join = jnp.where(col == kk * 64 + c * 32 + b * 8 + s, 1.0, 0.0).astype(BF)
            total = total + jnp.dot(value.astype(BF), join, preferred_element_type=F32)
        return jnp.dot(u[kk].reshape(512, 512), total.astype(BF), preferred_element_type=F32)

    build_table(f, 0)
    loads[0].wait()
    dft(0)
    pl.semaphore_wait(barrier, 24)
    y_send(0)
    build_table(f, 1)
    dft(1)
    y_send(1)

    col = lax.broadcasted_iota(jnp.int32, (1024, 128), 1)
    for b in range(8):
        perm[:, pl.ds(b * 128, 128)] = one_hot(
            (1024, 128), (col // 16) * 128 + (col % 8) * 16 + b * 2 + (col // 8) % 2
        )
    lane = lax.broadcasted_iota(jnp.int32, (512, 128), 1)
    slot40 = lax.broadcasted_iota(jnp.int32, (512, 40), 0)
    for kk in range(2):
        starts = start_ref[kk]
        total = jnp.max(starts + rank_ref[kk], axis=1, keepdims=True)
        begun = jnp.where(starts <= slot40, 1.0, 0.0) + jnp.where(total <= slot40, 64.0, 0.0)
        owner = jnp.sum(begun, axis=1, keepdims=True).astype(jnp.int32) - 1
        place[kk] = owner - 5 * (lane // 16)
    n = lax.broadcasted_iota(jnp.int32, (256, 256), 0)
    col = lax.broadcasted_iota(jnp.int32, (256, 256), 1)
    for c in range(2):
        source = ((n % 8) * 16 + n // 16) * 2 + c
        pick = jnp.where(col == source, 2.0, 0.0).astype(BF)
        for kk in range(2):
            table[kk * 2 + c] = jnp.dot(pick, f[kk], preferred_element_type=F32).astype(BF)

    g_send(0)
    for i in range(8):
        forward(0, i)
        if i >= 4:
            relay(0, i - 4)
    g_send(1)
    for i in range(8, 16):
        forward(0, i)
        relay(0, i - 4)
    for i in range(4):
        forward(1, i)
        relay(0, 12 + i)
    settle(0)
    for load in loads[1:]:
        load.wait()
    for jj in range(5):
        products(0, jj)
        for i in range(4 + 2 * jj, 6 + 2 * jj):
            forward(1, i)
            relay(1, i - 4)
    for i in range(14, 16):
        forward(1, i)
        relay(1, i - 4)
    e = coefficients(0)
    for i in range(12, 16):
        relay(1, i)
    settle(1)
    for jj in range(5):
        products(1, jj)
    e = e + coefficients(1)
    bb[...] = (e[:256] + swapped(e[256:], 32)).astype(BF)

    def y_back(i):
        d = YSTEPS[i]
        rows = pl.ds(pl.multiple_of(((y + d) % 8) * 32, 32), 32)
        return send(bb.at[rows], ry.at[y], f1s.at[i], f1r.at[i], y_peer(d))

    def g_back(i):
        d = STEPS[i]
        return send(pz.at[g_to(d)], rz.at[me_g], f2s.at[i], f2r.at[i], g_peer(d))

    for i in range(7):
        y_back(i).start()
    ry[y] = bb[pl.ds(pl.multiple_of(y * 32, 32), 32)]
    source = (n % 8) * 32 + (n // 16) * 2 + (n // 8) % 2
    pick = jnp.where(col == source, 1.0, 0.0).astype(BF)
    for i in range(7):
        y_back(i).wait_recv()
    moved = jnp.dot(pick, ry[...].reshape(256, 128), preferred_element_type=F32)
    pz[...] = moved.astype(BF).reshape(16, 16, 128)
    for i in range(15):
        g_back(i).start()
    rz[me_g] = pz[me_g]
    for i in range(15):
        g_back(i).wait_recv()
    turned = jnp.transpose(rz[...].reshape(256, 128).astype(F32))
    lane = lax.broadcasted_iota(jnp.int32, (32, 256), 1)
    series = jnp.zeros((64, 1024), F32)
    for b in range(4):
        part = turned[b * 32 : (b + 1) * 32]
        lhs = jnp.concatenate([jnp.where((lane // 8) % 2 == q, part, 0.0) for q in range(2)], axis=0)
        series = series + jnp.dot(lhs.astype(BF), table[b], preferred_element_type=F32)
    out_ref[...] = series.astype(BF)

    for kk in range(2):
        for i in range(7):
            y_copy(kk, i).wait_send()
        for i in range(15):
            g_copy(kk, i).wait_send()
        for a in range(2):
            whole(kk, x, xs.at[kk, a], x2.at[kk]).wait_send()
            whole(kk, x, xs2.at[kk, a], x2.at[kk], 640).wait_send()
    for i in range(7):
        y_back(i).wait_send()
    for i in range(15):
        g_back(i).wait_send()


VM = pl.BlockSpec(memory_space=pltpu.VMEM)
ANY = pl.BlockSpec(memory_space=pl.ANY)
DMA = pltpu.SemaphoreType.DMA


def per_device(wavefield, u_factors, v_factors, tile_ranks, tile_offsets):
    series = pl.pallas_call(
        kernel,
        out_shape=jax.ShapeDtypeStruct((64, 1024), BF),
        in_specs=[ANY, ANY, ANY, VM, VM],
        out_specs=VM,
        scratch_shapes=[
            pltpu.VMEM((640, 1024), BF),
            pltpu.VMEM((2, 2, 512, 256), BF),
            pltpu.VMEM((2, 2, 256, 512), BF),
            pltpu.VMEM((2, 256, 1024), BF),
            pltpu.VMEM((2, 640, 128), F32),
            pltpu.VMEM((2, 8, 80, 256), BF),
            pltpu.VMEM((2, 8, 80, 256), BF),
            pltpu.VMEM((1024, 1024), BF),
            pltpu.VMEM((2, 16, 80, 128), BF),
            pltpu.VMEM((4, 2, 1280, 128), BF),
            pltpu.VMEM((2, 512, 128), jnp.int32),
            pltpu.VMEM((1024, 512), F32),
            pltpu.VMEM((4, 256, 1024), BF),
            pltpu.VMEM((256, 128), BF),
            pltpu.VMEM((8, 32, 128), BF),
            pltpu.VMEM((16, 16, 128), BF),
            pltpu.VMEM((16, 16, 128), BF),
            DMA((5,)),
            DMA((2, 7)),
            DMA((2, 7)),
            DMA((2, 15)),
            DMA((2, 15)),
            DMA((2, 2)),
            DMA((2, 16)),
            DMA((2, 16)),
            DMA((2,)),
            DMA((2, 2)),
            DMA((7,)),
            DMA((7,)),
            DMA((15,)),
            DMA((15,)),
        ],
        compiler_params=pltpu.CompilerParams(
            collective_id=0, has_side_effects=True, vmem_limit_bytes=56 * 1024 * 1024
        ),
    )(wavefield.reshape(640, 1024), v_factors[:, :, 0], u_factors[:, :, 0], tile_ranks[:, 0:1], tile_offsets[:, 0:1])
    return series.reshape(2, 32, 1024)


def solution(mesh):
    torus = Mesh(
        mesh.devices.reshape(8, 8, 2, mesh.shape["rows"]), ("freq_0", "freq_1", "freq_2", "rows")
    )
    return jax.shard_map(
        per_device,
        mesh=torus,
        in_specs=(
            P(FREQ, "rows", None),
            P(None, FREQ, "rows", None, None),
            P(None, FREQ, "rows", None, None),
            P(FREQ, "rows", None),
            P(FREQ, "rows", None),
        ),
        out_specs=P(ROWS_FREQ, None, None),
        check_vma=False,
    )
```

```python
import math

import jax
import jax.numpy as jnp
import numpy as np
from jax import lax
from jax.experimental import pallas as pl
from jax.experimental.pallas import tpu as pltpu
from jax.sharding import Mesh
from jax.sharding import PartitionSpec as P

FREQ = ("freq_0", "freq_1", "freq_2")
ROWS_FREQ = ("rows", "freq_0", "freq_1", "freq_2")
BF = jnp.bfloat16
F32 = jnp.float32
MESH = pl.DeviceIdType.MESH

_z = 0.125 * (1.0 - np.cos(np.pi * (np.arange(64) + 0.5) / 64))
COS = [float(a) for a in np.polynomial.polynomial.polyfit(_z, np.cos(2 * np.pi * np.sqrt(_z)), 9)]

STEPS = [(0, 1)] + [(d, c) for d in (1, 7, 4, 3, 5, 2, 6) for c in (0, 1)]
YSTEPS = (4, 3, 5, 2, 6, 1, 7)


def cosine(m):
    x = jnp.where(m >= 512, m - 1024, m).astype(F32) * (1.0 / 1024.0)
    z = x * x
    value = jnp.full(m.shape, COS[-1], F32)
    for a in COS[-2::-1]:
        value = value * z + a
    return value


def build_table(f_ref, kk):
    for part in range(4):
        row = lax.broadcasted_iota(jnp.int32, (64, 128), 0) + part * 64
        lane = lax.broadcasted_iota(jnp.int32, (64, 128), 1)
        k1 = (row // 2) * 2 + (kk + 1)
        m = (k1 * lane + (row % 2) * 256) & 1023
        co, si = cosine(m), cosine((m + 768) & 1023)
        turn = (k1 * 128) & 1023
        ct, st = cosine(turn), cosine((turn + 768) & 1023)
        for b in range(8):
            f_ref[kk, pl.ds(part * 64, 64), pl.ds(b * 128, 128)] = (co * (1.0 / 32.0)).astype(BF)
            if b < 7:
                co, si = co * ct - si * st, si * ct + co * st


def one_hot(shape, source):
    row = lax.broadcasted_iota(jnp.int32, shape, 0)
    return jnp.where(row == source, 1.0, 0.0).astype(BF)


def swapped(b, width):
    lane = lax.broadcasted_iota(jnp.int32, b.shape, 1)
    real = (lane // width) % 2 == 0
    return jnp.where(real, -pltpu.roll(b, b.shape[1] - width, axis=1), pltpu.roll(b, width, axis=1))


def kernel(
    w_hbm, v_hbm, u_hbm, rank_ref, start_ref, out_ref,
    w, v, vg, u, f, o, s1, r1, perm, pack, unpack, p2, g, mine, meta, place, place4, acc, cs, cr,
    table, bb, ry, pz, rz,
    load_sem, s1s, r1s, p2s, p2r, xs, xm, xp, x2, xs2, f1s, f1r, f2s, f2r,
    vs, vm, vp, v2, vs2, ms, mr, css, crs,
):
    y = lax.axis_index("freq_0")
    z = lax.axis_index("freq_1")
    core = lax.axis_index("freq_2")
    x = lax.axis_index("rows")
    me_g = z * 2 + core

    loads = [
        pltpu.make_async_copy(w_hbm, w, load_sem.at[0]),
        pltpu.make_async_copy(v_hbm.at[:, 1], vg.at[x], load_sem.at[1]),
        pltpu.make_async_copy(v_hbm.at[:, 0], v, load_sem.at[2]),
        pltpu.make_async_copy(u_hbm.at[:, 0], u.at[0], load_sem.at[3]),
        pltpu.make_async_copy(u_hbm.at[:, 1], u.at[1], load_sem.at[4]),
    ]
    for load in loads:
        load.start()

    def y_peer(d):
        return {"freq_0": (y + d) % 8}

    def g_peer(d):
        return {"freq_1": (z + d[0]) % 8, "freq_2": (core + d[1]) % 2}

    def g_to(d):
        return ((z + d[0]) % 8) * 2 + (core + d[1]) % 2

    def g_from(d):
        return ((z + 8 - d[0]) % 8) * 2 + (core + 2 - d[1]) % 2

    x_up, x_down = (x + 1) % 4, (x + 3) % 4

    barrier = pltpu.get_barrier_semaphore()
    for d in YSTEPS:
        pl.semaphore_signal(barrier, inc=1, device_id=y_peer(d), device_id_type=MESH)
    for d in STEPS:
        pl.semaphore_signal(barrier, inc=1, device_id=g_peer(d), device_id_type=MESH)
    for peer in (x_up, x_down, (x + 2) % 4):
        pl.semaphore_signal(barrier, inc=1, device_id={"rows": peer}, device_id_type=MESH)

    def send(src, dst, ssem, rsem, peer):
        return pltpu.make_async_remote_copy(
            src_ref=src, dst_ref=dst, send_sem=ssem, recv_sem=rsem, device_id=peer, device_id_type=MESH
        )

    def y_copy(kk, i):
        d = YSTEPS[i]
        return send(s1.at[kk, (y + d) % 8], r1.at[kk, y], s1s.at[kk, i], r1s.at[kk, i], y_peer(d))

    def g_copy(kk, i):
        d = STEPS[i]
        rows = pl.ds(me_g * 80, 80)
        return send(p2.at[kk, g_to(d)], g.at[x, kk, rows], p2s.at[kk, i], p2r.at[kk, i], g_peer(d))

    def block(kk, i, owner):
        gs = me_g if i == 0 else g_from(STEPS[i - 1])
        return g.at[owner, kk, pl.ds(gs * 80, 80)]

    def x_copy(kk, i, up):
        ref = block(kk, i, x)
        if up:
            return send(ref, ref, xs.at[kk, 0], xm.at[kk, i], {"rows": x_up})
        return send(ref, ref, xs.at[kk, 1], xp.at[kk, i], {"rows": x_down})

    def x_relay(kk, i):
        if i % 2 == 0:
            ref = block(kk, i, x_down)
            return send(ref, ref, xs2.at[kk, 0], x2.at[kk], {"rows": x_up})
        ref = block(kk, i, x_up)
        return send(ref, ref, xs2.at[kk, 1], x2.at[kk], {"rows": x_down})

    def v_copy(a, up):
        ref = vg.at[x, a // 2, pl.ds((a % 2) * 256, 256)]
        if up:
            return send(ref, ref, vs.at[0], vm.at[a], {"rows": x_up})
        return send(ref, ref, vs.at[1], vp.at[a], {"rows": x_down})

    def v_relay(a):
        rows = pl.ds((a % 2) * 256, 256)
        if a < 2:
            ref = vg.at[x_down, a // 2, rows]
            return send(ref, ref, vs2.at[0], v2, {"rows": x_up})
        ref = vg.at[x_up, a // 2, rows]
        return send(ref, ref, vs2.at[1], v2, {"rows": x_down})

    def v_pass(a):
        v_copy(a, a < 2).wait_recv()
        v_relay(a).start()

    def meta_copy(d):
        return send(mine, meta.at[x], ms.at[d - 1], mr.at[d - 1], {"rows": (x + d) % 4})

    def coeff_copy(d):
        return send(cs.at[(x + d) % 4], cr.at[x], css.at[d - 1], crs.at[d - 1], {"rows": (x + d) % 4})

    def v_whole(ssem, rsem, part):
        ref = vg.at[x] if part is None else vg.at[x, part]
        return send(ref, ref, ssem, rsem, {"rows": x_up})

    def dft(kk):
        for half in range(2):
            o[half] = lax.dot_general(
                w[...], f[kk, pl.ds(half * 128, 128)], (((1,), (1,)), ((), ())), preferred_element_type=F32
            )
        slot = lax.broadcasted_iota(jnp.int32, (16, 128), 1) // 16

        def place_rows(chunk, carry):
            for half in range(2):
                turned = []
                for s in range(8):
                    t = o[half, pl.ds(chunk * 128 + s, 16, stride=8), :]
                    turned.append(pltpu.roll(t, 16 * s, axis=1) if s else t)
                for b in range(8):
                    value = turned[(-b) % 8]
                    for q in range(1, 8):
                        value = jnp.where(slot == q, turned[(q - b) % 8], value)
                    rows = pl.ds(pl.multiple_of(chunk * 16, 16), 16)
                    s1[kk, half * 4 + b // 2, rows, pl.ds((b % 2) * 128, 128)] = value.astype(BF)
            return carry

        lax.fori_loop(0, 5, place_rows, 0)

    def y_send(kk):
        for i in range(7):
            y_copy(kk, i).start()
        r1[kk, y] = s1[kk, y]

    def g_send(kk):
        for i in range(7):
            y_copy(kk, i).wait_recv()
        lhs = jnp.concatenate(
            [
                jnp.concatenate([r1[kk, a, :, pl.ds(h * 128, 128)] for a in range(8)], axis=1)
                for h in range(2)
            ],
            axis=0,
        )
        for b in range(8):
            moved = jnp.dot(lhs, perm[:, pl.ds(b * 128, 128)], preferred_element_type=F32).astype(BF)
            p2[kk, b] = moved[:80]
            p2[kk, 8 + b] = moved[80:]
        for i in range(15):
            g_copy(kk, i).start()
        g[x, kk, pl.ds(pl.multiple_of(me_g * 80, 16), 80)] = p2[kk, me_g]

    def forward(kk, i):
        if i > 0:
            g_copy(kk, i - 1).wait_recv()
        x_copy(kk, i, True).start()
        x_copy(kk, i, False).start()

    def relay(kk, i):
        x_copy(kk, i, i % 2 == 0).wait_recv()
        x_relay(kk, i).start()

    def whole(kk, owner, ssem, rsem, rows=1280):
        ref = g.at[owner, kk, pl.ds(0, rows)]
        return send(ref, ref, ssem, rsem, {"rows": x_up})

    def settle(kk):
        for i in range(16):
            x_copy(kk, i, i % 2 == 1).wait_recv()
        whole(kk, x, xs.at[kk, 0], x2.at[kk]).wait_recv()

    def products(jj):
        for half in range(2):
            rows = pl.ds(jj * 256, 256)
            rhs = jnp.concatenate([g[2 * half, 0, rows, :], g[2 * half + 1, 0, rows, :]], axis=1)
            prod = jnp.dot(v[...].reshape(1024, 256), rhs, preferred_element_type=F32)
            for m in range(2):
                hit = place[...] == jj
                lanes = pl.ds((2 * half + m) * 128, 128)
                for ab in range(2):
                    old = acc[pl.ds(ab * 512, 512), lanes] if jj else 0.0
                    new = prod[ab * 512 : (ab + 1) * 512, m * 128 : (m + 1) * 128]
                    acc[pl.ds(ab * 512, 512), lanes] = jnp.where(hit, new, old)

    def coefficients():
        row = lax.broadcasted_iota(jnp.int32, (128, 128), 0)
        col = lax.broadcasted_iota(jnp.int32, (128, 128), 1)
        c, s = (row // 8) % 2, (row % 8 + 8 - turn) % 8
        total = jnp.zeros((512, 128), F32)
        for b in range(4):
            lanes = pl.ds(b * 128, 128)
            value = acc[pl.ds(0, 512), lanes] + swapped(acc[pl.ds(512, 512), lanes], 8)
            join = jnp.where(col == c * 32 + b * 8 + s, 1.0, 0.0).astype(BF)
            total = total + jnp.dot(value.astype(BF), join, preferred_element_type=F32)
        return total.astype(BF)

    def own_products():
        lhs = []
        for row in range(4):
            factors = vg[row].reshape(1024, 256)
            for pair in ((0, 1), (2, 3), (4,)):
                rhs = jnp.concatenate([g[x, 1, pl.ds(jj * 256, 256), :] for jj in pair], axis=1)
                prod = jnp.dot(factors, rhs, preferred_element_type=F32)
                for m, jj in enumerate(pair):
                    hit = place4[row] == jj
                    for ab in range(2):
                        rows = pl.ds(ab * 512, 512)
                        old = acc[rows, pl.ds(row * 128, 128)] if jj else 0.0
                        new = prod[ab * 512 : (ab + 1) * 512, m * 128 : (m + 1) * 128]
                        acc[rows, pl.ds(row * 128, 128)] = jnp.where(hit, new, old)
            lanes = pl.ds(row * 128, 128)
            value = (acc[pl.ds(0, 512), lanes] + swapped(acc[pl.ds(512, 512), lanes], 8)).astype(BF)
            lhs.append(jnp.concatenate([value[a * 64 : (a + 1) * 64] for a in range(8)], axis=1))
        packed = jnp.dot(jnp.concatenate(lhs, axis=0), pack[...], preferred_element_type=F32).astype(BF)
        for row in range(4):
            cs[row] = packed[row * 64 : (row + 1) * 64]
        for d in range(1, 4):
            coeff_copy(d).start()
        cr[x] = cs[x]

    def other_coefficients():
        for d in range(1, 4):
            coeff_copy(d).wait_recv()
        lhs = jnp.concatenate([cr[a] for a in range(4)], axis=1)
        wide = jnp.dot(lhs, unpack[...], preferred_element_type=F32).astype(BF)
        return jnp.concatenate([wide[:, a * 128 : (a + 1) * 128] for a in range(8)], axis=0)

    turn = (y % 4) * 2 + z // 4

    build_table(f, 0)
    loads[0].wait()
    dft(0)
    pl.semaphore_wait(barrier, 25)
    y_send(0)
    mine[...] = jnp.full((8, 128), 1e9, F32)
    mine[0:1, 0:40] = start_ref[1].astype(F32)
    mine[0:1, 40:41] = jnp.max(start_ref[1] + rank_ref[1], axis=1, keepdims=True).astype(F32)
    for d in range(1, 4):
        meta_copy(d).start()
    meta[x] = mine[...]
    loads[1].wait()
    for a in range(4):
        v_copy(a, True).start()
        v_copy((a + 2) % 4, False).start()
    build_table(f, 1)
    dft(1)
    y_send(1)

    col = lax.broadcasted_iota(jnp.int32, (1024, 128), 1)
    for b in range(8):
        perm[:, pl.ds(b * 128, 128)] = one_hot(
            (1024, 128), (col // 16) * 128 + (col % 8) * 16 + b * 2 + (col // 8) % 2
        )
    lane = lax.broadcasted_iota(jnp.int32, (512, 128), 1)
    slot40 = lax.broadcasted_iota(jnp.int32, (512, 40), 0)
    starts = start_ref[0]
    total = jnp.max(starts + rank_ref[0], axis=1, keepdims=True)
    begun = jnp.where(starts <= slot40, 1.0, 0.0) + jnp.where(total <= slot40, 64.0, 0.0)
    owner = jnp.sum(begun, axis=1, keepdims=True).astype(jnp.int32) - 1
    place[...] = owner - 5 * (lane // 16)
    row = lax.broadcasted_iota(jnp.int32, (1024, 128), 0)
    col = lax.broadcasted_iota(jnp.int32, (1024, 128), 1)
    pack[...] = jnp.where(col == (row // 128) * 16 + row % 16, 1.0, 0.0).astype(BF)
    row = lax.broadcasted_iota(jnp.int32, (512, 128), 0)
    col = lax.broadcasted_iota(jnp.int32, (512, 128), 1)
    target = 64 + ((row // 8) % 2) * 32 + (row // 128) * 8 + (row % 8 + 8 - turn) % 8
    for a in range(8):
        hit = (col == target) & ((row // 16) % 8 == a)
        unpack[:, pl.ds(a * 128, 128)] = jnp.where(hit, 1.0, 0.0).astype(BF)
    n = lax.broadcasted_iota(jnp.int32, (256, 256), 0)
    col = lax.broadcasted_iota(jnp.int32, (256, 256), 1)
    for c in range(2):
        source = ((n % 8) * 16 + n // 16) * 2 + c
        pick = jnp.where(col == source, 2.0, 0.0).astype(BF)
        for kk in range(2):
            table[kk * 2 + c] = jnp.dot(pick, f[kk], preferred_element_type=F32).astype(BF)

    for d in range(1, 4):
        meta_copy(d).wait_recv()
    slot = lax.broadcasted_iota(jnp.int32, (512, 128), 0).astype(F32)
    weight = jnp.where(lane == 40, 64.0, 1.0)
    for row in range(4):
        begun = jnp.where(meta[row, 0:1, :] <= slot, weight, 0.0)
        owner = jnp.sum(begun, axis=1, keepdims=True).astype(jnp.int32) - 1
        place4[row] = owner - 5 * (lane // 16)
    for a in (0, 2, 1, 3):
        v_pass(a)
    g_send(0)
    for i in range(8):
        forward(0, i)
    g_send(1)
    for i in range(8, 16):
        forward(0, i)
    for i in range(16):
        relay(0, i)
    for a in range(4):
        v_copy(a, a >= 2).wait_recv()
    v_whole(vs.at[0], v2, None).wait_recv()
    for i in range(15):
        g_copy(1, i).wait_recv()
    own_products()
    for load in loads[2:]:
        load.wait()
    settle(0)
    for jj in range(5):
        products(jj)
    e = jnp.dot(u[0].reshape(512, 512), coefficients(), preferred_element_type=F32)
    e = e + jnp.dot(u[1].reshape(512, 512), other_coefficients(), preferred_element_type=F32)
    bb[...] = (e[:256] + swapped(e[256:], 32)).astype(BF)

    def y_back(i):
        d = YSTEPS[i]
        rows = pl.ds(pl.multiple_of(((y + d) % 8) * 32, 32), 32)
        return send(bb.at[rows], ry.at[y], f1s.at[i], f1r.at[i], y_peer(d))

    def g_back(i):
        d = STEPS[i]
        return send(pz.at[g_to(d)], rz.at[me_g], f2s.at[i], f2r.at[i], g_peer(d))

    for i in range(7):
        y_back(i).start()
    ry[y] = bb[pl.ds(pl.multiple_of(y * 32, 32), 32)]
    source = (n % 8) * 32 + (n // 16) * 2 + (n // 8) % 2
    pick = jnp.where(col == source, 1.0, 0.0).astype(BF)
    for i in range(7):
        y_back(i).wait_recv()
    moved = jnp.dot(pick, ry[...].reshape(256, 128), preferred_element_type=F32)
    pz[...] = moved.astype(BF).reshape(16, 16, 128)
    for i in range(15):
        g_back(i).start()
    rz[me_g] = pz[me_g]
    for i in range(15):
        g_back(i).wait_recv()
    turned = jnp.transpose(rz[...].reshape(256, 128).astype(F32))
    lane = lax.broadcasted_iota(jnp.int32, (32, 256), 1)
    series = jnp.zeros((64, 1024), F32)
    for b in range(4):
        part = turned[b * 32 : (b + 1) * 32]
        lhs = jnp.concatenate([jnp.where((lane // 8) % 2 == q, part, 0.0) for q in range(2)], axis=0)
        series = series + jnp.dot(lhs.astype(BF), table[b], preferred_element_type=F32)
    out_ref[...] = series.astype(BF)

    for kk in range(2):
        for i in range(7):
            y_copy(kk, i).wait_send()
        for i in range(15):
            g_copy(kk, i).wait_send()
    for a in range(2):
        whole(0, x, xs.at[0, a], x2.at[0]).wait_send()
        whole(0, x, xs2.at[0, a], x2.at[0], 640).wait_send()
        v_whole(vs.at[a], v2, None).wait_send()
        v_whole(vs2.at[a], v2, 0).wait_send()
    for d in range(1, 4):
        meta_copy(d).wait_send()
        coeff_copy(d).wait_send()
    for i in range(7):
        y_back(i).wait_send()
    for i in range(15):
        g_back(i).wait_send()


VM = pl.BlockSpec(memory_space=pltpu.VMEM)
ANY = pl.BlockSpec(memory_space=pl.ANY)
DMA = pltpu.SemaphoreType.DMA


def per_device(wavefield, u_factors, v_factors, tile_ranks, tile_offsets):
    series = pl.pallas_call(
        kernel,
        out_shape=jax.ShapeDtypeStruct((64, 1024), BF),
        in_specs=[ANY, ANY, ANY, VM, VM],
        out_specs=VM,
        scratch_shapes=[
            pltpu.VMEM((640, 1024), BF),
            pltpu.VMEM((2, 512, 256), BF),
            pltpu.VMEM((4, 2, 512, 256), BF),
            pltpu.VMEM((2, 2, 256, 512), BF),
            pltpu.VMEM((2, 256, 1024), BF),
            pltpu.VMEM((2, 640, 128), F32),
            pltpu.VMEM((2, 8, 80, 256), BF),
            pltpu.VMEM((2, 8, 80, 256), BF),
            pltpu.VMEM((1024, 1024), BF),
            pltpu.VMEM((1024, 128), BF),
            pltpu.VMEM((512, 1024), BF),
            pltpu.VMEM((2, 16, 80, 128), BF),
            pltpu.VMEM((4, 2, 1280, 128), BF),
            pltpu.VMEM((8, 128), F32),
            pltpu.VMEM((4, 8, 128), F32),
            pltpu.VMEM((512, 128), jnp.int32),
            pltpu.VMEM((4, 512, 128), jnp.int32),
            pltpu.VMEM((1024, 512), F32),
            pltpu.VMEM((4, 64, 128), BF),
            pltpu.VMEM((4, 64, 128), BF),
            pltpu.VMEM((4, 256, 1024), BF),
            pltpu.VMEM((256, 128), BF),
            pltpu.VMEM((8, 32, 128), BF),
            pltpu.VMEM((16, 16, 128), BF),
            pltpu.VMEM((16, 16, 128), BF),
            DMA((5,)),
            DMA((2, 7)),
            DMA((2, 7)),
            DMA((2, 15)),
            DMA((2, 15)),
            DMA((2, 2)),
            DMA((2, 16)),
            DMA((2, 16)),
            DMA((2,)),
            DMA((2, 2)),
            DMA((7,)),
            DMA((7,)),
            DMA((15,)),
            DMA((15,)),
            DMA((2,)),
            DMA((4,)),
            DMA((4,)),
            DMA,
            DMA((2,)),
            DMA((3,)),
            DMA((3,)),
            DMA((3,)),
            DMA((3,)),
        ],
        compiler_params=pltpu.CompilerParams(
            collective_id=0, has_side_effects=True, vmem_limit_bytes=56 * 1024 * 1024
        ),
    )(wavefield.reshape(640, 1024), v_factors[:, :, 0], u_factors[:, :, 0], tile_ranks[:, 0:1], tile_offsets[:, 0:1])
    return series.reshape(2, 32, 1024)


def solution(mesh):
    torus = Mesh(
        mesh.devices.reshape(8, 8, 2, mesh.shape["rows"]), ("freq_0", "freq_1", "freq_2", "rows")
    )
    return jax.shard_map(
        per_device,
        mesh=torus,
        in_specs=(
            P(FREQ, "rows", None),
            P(None, FREQ, "rows", None, None),
            P(None, FREQ, "rows", None, None),
            P(FREQ, "rows", None),
            P(FREQ, "rows", None),
        ),
        out_specs=P(ROWS_FREQ, None, None),
        check_vma=False,
    )
```

```python
import math

import jax
import jax.numpy as jnp
import numpy as np
from jax import lax
from jax.experimental import pallas as pl
from jax.experimental.pallas import tpu as pltpu
from jax.sharding import Mesh
from jax.sharding import PartitionSpec as P

FREQ = ("freq_0", "freq_1", "freq_2")
ROWS_FREQ = ("rows", "freq_0", "freq_1", "freq_2")
BF = jnp.bfloat16
F32 = jnp.float32
MESH = pl.DeviceIdType.MESH

_z = 0.125 * (1.0 - np.cos(np.pi * (np.arange(64) + 0.5) / 64))
COS = [float(a) for a in np.polynomial.polynomial.polyfit(_z, np.cos(2 * np.pi * np.sqrt(_z)), 9)]

STEPS = [(0, 1)] + [(d, c) for d in (1, 7, 4, 5, 3, 2, 6) for c in (0, 1)]
YSTEPS = (4, 3, 5, 2, 6, 1, 7)


def cosine(m):
    x = jnp.where(m >= 512, m - 1024, m).astype(F32) * (1.0 / 1024.0)
    z = x * x
    value = jnp.full(m.shape, COS[-1], F32)
    for a in COS[-2::-1]:
        value = value * z + a
    return value


def build_table(f_ref, kk):
    for part in range(4):
        row = lax.broadcasted_iota(jnp.int32, (64, 128), 0) + part * 64
        lane = lax.broadcasted_iota(jnp.int32, (64, 128), 1)
        k1 = (row // 2) * 2 + (kk + 1)
        m = (k1 * lane + (row % 2) * 256) & 1023
        co, si = cosine(m), cosine((m + 768) & 1023)
        turn = (k1 * 128) & 1023
        ct, st = cosine(turn), cosine((turn + 768) & 1023)
        for b in range(8):
            f_ref[kk, pl.ds(part * 64, 64), pl.ds(b * 128, 128)] = (co * (1.0 / 32.0)).astype(BF)
            if b < 7:
                co, si = co * ct - si * st, si * ct + co * st


def one_hot(shape, source):
    row = lax.broadcasted_iota(jnp.int32, shape, 0)
    return jnp.where(row == source, 1.0, 0.0).astype(BF)


def swapped(b, width):
    lane = lax.broadcasted_iota(jnp.int32, b.shape, 1)
    real = (lane // width) % 2 == 0
    return jnp.where(real, -pltpu.roll(b, b.shape[1] - width, axis=1), pltpu.roll(b, width, axis=1))


def kernel(
    w_hbm, v_hbm, u_hbm, rank_hbm, start_hbm, out_ref,
    rank_ref, start_ref, w, v, vg, u, f, o, s1, r1, perm, pack, unpack, p2, g, mine, meta, place, place4, acc, cs, cr,
    table, bb, ry, pz, rz,
    load_sem, s1s, r1s, p2s, p2r, xs, xm, xp, x2, xs2, fs,
    vs, vm, vp, v2, vs2, ms, mr, css, crs,
):
    y = lax.axis_index("freq_0")
    z = lax.axis_index("freq_1")
    core = lax.axis_index("freq_2")
    x = lax.axis_index("rows")
    me_g = z * 2 + core

    loads = [
        pltpu.make_async_copy(w_hbm, w, load_sem.at[0]),
        pltpu.make_async_copy(v_hbm.at[:, 1], vg.at[x], load_sem.at[1]),
        pltpu.make_async_copy(v_hbm.at[:, 0], v, load_sem.at[2]),
        pltpu.make_async_copy(u_hbm.at[:, 0], u.at[0], load_sem.at[3]),
        pltpu.make_async_copy(u_hbm.at[:, 1], u.at[1], load_sem.at[4]),
        pltpu.make_async_copy(rank_hbm, rank_ref, load_sem.at[5]),
        pltpu.make_async_copy(start_hbm, start_ref, load_sem.at[6]),
    ]
    for load in loads:
        load.start()

    def y_peer(d):
        return {"freq_0": (y + d) % 8}

    def g_peer(d):
        return {"freq_1": (z + d[0]) % 8, "freq_2": (core + d[1]) % 2}

    def g_to(d):
        return ((z + d[0]) % 8) * 2 + (core + d[1]) % 2

    def g_from(d):
        return ((z + 8 - d[0]) % 8) * 2 + (core + 2 - d[1]) % 2

    x_up, x_down = (x + 1) % 4, (x + 3) % 4

    barrier = pltpu.get_barrier_semaphore()
    for d in YSTEPS:
        pl.semaphore_signal(barrier, inc=1, device_id=y_peer(d), device_id_type=MESH)
    for d in STEPS:
        pl.semaphore_signal(barrier, inc=1, device_id=g_peer(d), device_id_type=MESH)
    for peer in (x_up, x_down, (x + 2) % 4):
        pl.semaphore_signal(barrier, inc=1, device_id={"rows": peer}, device_id_type=MESH)

    def send(src, dst, ssem, rsem, peer):
        return pltpu.make_async_remote_copy(
            src_ref=src, dst_ref=dst, send_sem=ssem, recv_sem=rsem, device_id=peer, device_id_type=MESH
        )

    def y_copy(kk, i):
        d = YSTEPS[i]
        return send(s1.at[kk, (y + d) % 8], r1.at[kk, y], s1s.at[kk], r1s.at[kk], y_peer(d))

    def y_all(kk):
        ref = r1.at[kk, pl.ds(0, 7)]
        return send(ref, ref, s1s.at[kk], r1s.at[kk], y_peer(1))

    def g_copy(kk, i):
        d = STEPS[i]
        rows = pl.ds(me_g * 80, 80)
        return send(p2.at[kk, g_to(d)], g.at[x, kk, rows], p2s.at[kk], p2r.at[15 if kk else i], g_peer(d))

    def g_all(kk):
        ref = g.at[x, kk, pl.ds(0, 1200)]
        return send(ref, ref, p2s.at[kk], p2r.at[15], g_peer(STEPS[0]))

    def block(gs, owner):
        return g.at[owner, 0, pl.ds(gs * 80, 80)]

    def x_copy(gs, up):
        ref = block(gs, x)
        if up:
            return send(ref, ref, xs.at[0], xm.at[8 - (8 - gs // 2) * (1 - gs % 2)], {"rows": x_up})
        return send(ref, ref, xs.at[1], xp.at[8 - (8 - gs // 2) * (gs % 2)], {"rows": x_down})

    def x_relay(gs):
        if gs % 2 == 0:
            ref = block(gs, x_down)
            return send(ref, ref, xs2.at[0], x2.at[gs // 4], {"rows": x_up})
        ref = block(gs, x_up)
        return send(ref, ref, xs2.at[1], x2.at[gs // 4], {"rows": x_down})

    def v_copy(a, up):
        ref = vg.at[x, a // 2, pl.ds((a % 2) * 256, 256)]
        if up:
            return send(ref, ref, vs.at[0], vm.at[a], {"rows": x_up})
        return send(ref, ref, vs.at[1], vp.at[a], {"rows": x_down})

    def v_relay(a):
        rows = pl.ds((a % 2) * 256, 256)
        if a < 2:
            ref = vg.at[x_down, a // 2, rows]
            return send(ref, ref, vs2.at[0], v2, {"rows": x_up})
        ref = vg.at[x_up, a // 2, rows]
        return send(ref, ref, vs2.at[1], v2, {"rows": x_down})

    def v_pass(a):
        v_copy(a, a < 2).wait_recv()
        v_relay(a).start()

    def meta_copy(d):
        return send(mine, meta.at[x], ms, mr, {"rows": (x + d) % 4})

    meta_all = send(meta.at[pl.ds(0, 3)], meta.at[pl.ds(0, 3)], ms, mr, {"rows": x_up})

    def coeff_copy(d):
        return send(cs.at[(x + d) % 4], cr.at[x], css, crs, {"rows": (x + d) % 4})

    coeffs_all = send(cs.at[pl.ds(0, 3)], cr.at[pl.ds(0, 3)], css, crs, {"rows": x_up})

    def v_whole(ssem, rsem, part):
        ref = vg.at[x] if part is None else vg.at[x, part]
        return send(ref, ref, ssem, rsem, {"rows": x_up})

    def dft(kk):
        for half in range(2):
            o[half] = lax.dot_general(
                w[...], f[kk, pl.ds(half * 128, 128)], (((1,), (1,)), ((), ())), preferred_element_type=F32
            )
        slot = lax.broadcasted_iota(jnp.int32, (16, 128), 1) // 16

        def place_rows(chunk, carry):
            for half in range(2):
                turned = []
                for s in range(8):
                    t = o[half, pl.ds(chunk * 128 + s, 16, stride=8), :]
                    turned.append(pltpu.roll(t, 16 * s, axis=1) if s else t)
                for b in range(8):
                    value = turned[(-b) % 8]
                    for q in range(1, 8):
                        value = jnp.where(slot == q, turned[(q - b) % 8], value)
                    rows = pl.ds(pl.multiple_of(chunk * 16, 16), 16)
                    s1[kk, half * 4 + b // 2, rows, pl.ds((b % 2) * 128, 128)] = value.astype(BF)
            return carry

        lax.fori_loop(0, 5, place_rows, 0)

    def y_send(kk):
        for i in range(7):
            y_copy(kk, i).start()
        r1[kk, y] = s1[kk, y]

    def g_send(kk):
        y_all(kk).wait_recv()
        lhs = jnp.concatenate(
            [
                jnp.concatenate([r1[kk, a, :, pl.ds(h * 128, 128)] for a in range(8)], axis=1)
                for h in range(2)
            ],
            axis=0,
        )
        for dz in (0, 1, 3, 2):
            b = ((z + dz) % 4) * 2
            cols = pl.ds(pl.multiple_of(b * 128, 256), 256)
            moved = jnp.dot(lhs, perm[:, cols], preferred_element_type=F32).astype(BF)
            for c in range(2):
                p2[kk, b + c] = moved[:80, c * 128 : (c + 1) * 128]
                p2[kk, 8 + b + c] = moved[80:, c * 128 : (c + 1) * 128]
            for d in (dz, dz + 4):
                for dc in (1, 0):
                    if (d, dc) == (0, 0):
                        g[x, kk, pl.ds(pl.multiple_of(me_g * 80, 16), 80)] = p2[kk, me_g]
                    else:
                        g_copy(kk, STEPS.index((d, dc))).start()

    def forward(i):
        gs = me_g
        if i > 0:
            g_copy(0, i - 1).wait_recv()
            gs = g_from(STEPS[i - 1])
        x_copy(gs, True).start()
        x_copy(gs, False).start()

    def relay(gs):
        x_copy(gs, gs % 2 == 0).wait_recv()
        x_relay(gs).start()

    def whole(kk, owner, ssem, rsem, rows=1280):
        ref = g.at[owner, kk, pl.ds(0, rows)]
        return send(ref, ref, ssem, rsem, {"rows": x_up})

    def settle():
        whole(0, x, xs.at[0], xm.at[8], 640).wait_recv()
        whole(0, x, xs.at[0], xp.at[8], 640).wait_recv()

    def products(jj):
        for half in range(2):
            rows = pl.ds(jj * 256, 256)
            rhs = jnp.concatenate([g[2 * half, 0, rows, :], g[2 * half + 1, 0, rows, :]], axis=1)
            prod = jnp.dot(v[...].reshape(1024, 256), rhs, preferred_element_type=F32)
            for m in range(2):
                hit = place[...] == jj
                lanes = pl.ds((2 * half + m) * 128, 128)
                for ab in range(2):
                    old = acc[pl.ds(ab * 512, 512), lanes] if jj else 0.0
                    new = prod[ab * 512 : (ab + 1) * 512, m * 128 : (m + 1) * 128]
                    acc[pl.ds(ab * 512, 512), lanes] = jnp.where(hit, new, old)

    def coefficients():
        row = lax.broadcasted_iota(jnp.int32, (128, 128), 0)
        col = lax.broadcasted_iota(jnp.int32, (128, 128), 1)
        c, s = (row // 8) % 2, (row % 8 + 8 - turn) % 8
        total = jnp.zeros((512, 128), F32)
        for b in range(4):
            lanes = pl.ds(b * 128, 128)
            value = acc[pl.ds(0, 512), lanes] + swapped(acc[pl.ds(512, 512), lanes], 8)
            join = jnp.where(col == c * 32 + b * 8 + s, 1.0, 0.0).astype(BF)
            total = total + jnp.dot(value.astype(BF), join, preferred_element_type=F32)
        return total.astype(BF)

    def own_products():
        pairs = ((0, 1), (2, 3), (4,))
        for d in (2, 1, 3, 0):
            row = (x + d) % 4
            factors = vg[row].reshape(1024, 256)
            lanes = pl.ds(d * 128, 128)
            for pair in pairs:
                rhs = jnp.concatenate([g[x, 1, pl.ds(jj * 256, 256), :] for jj in pair], axis=1)
                prod = jnp.dot(factors, rhs, preferred_element_type=F32)
                for m, jj in enumerate(pair):
                    hit = place4[row] == jj
                    for ab in range(2):
                        rows = pl.ds(ab * 512, 512)
                        old = acc[rows, lanes] if jj else 0.0
                        new = prod[ab * 512 : (ab + 1) * 512, m * 128 : (m + 1) * 128]
                        acc[rows, lanes] = jnp.where(hit, new, old)
            value = (acc[pl.ds(0, 512), lanes] + swapped(acc[pl.ds(512, 512), lanes], 8)).astype(BF)
            wide = jnp.concatenate([value[a * 64 : (a + 1) * 64] for a in range(8)], axis=1)
            cs[row] = jnp.dot(wide, pack[...], preferred_element_type=F32).astype(BF)
            if d:
                coeff_copy(d).start()
            else:
                cr[x] = cs[x]

    def other_coefficients():
        coeffs_all.wait_recv()
        lhs = jnp.concatenate([cr[a] for a in range(4)], axis=1)
        wide = jnp.dot(lhs, unpack[...], preferred_element_type=F32).astype(BF)
        return jnp.concatenate([wide[:, a * 128 : (a + 1) * 128] for a in range(8)], axis=0)

    turn = (y % 4) * 2 + z // 4

    build_table(f, 0)
    loads[0].wait()
    dft(0)
    pl.semaphore_wait(barrier, 25)
    y_send(0)
    loads[5].wait()
    loads[6].wait()
    mine[...] = jnp.full((8, 128), 1e9, F32)
    mine[0:1, 0:40] = start_ref[1].astype(F32)
    mine[0:1, 40:41] = jnp.max(start_ref[1] + rank_ref[1], axis=1, keepdims=True).astype(F32)
    for d in range(1, 4):
        meta_copy(d).start()
    meta[x] = mine[...]
    loads[1].wait()
    for a in range(4):
        v_copy(a, True).start()
        v_copy((a + 2) % 4, False).start()
    build_table(f, 1)
    dft(1)
    y_send(1)

    col = lax.broadcasted_iota(jnp.int32, (1024, 128), 1)
    for b in range(8):
        perm[:, pl.ds(b * 128, 128)] = one_hot(
            (1024, 128), (col // 16) * 128 + (col % 8) * 16 + b * 2 + (col // 8) % 2
        )
    lane = lax.broadcasted_iota(jnp.int32, (512, 128), 1)
    slot40 = lax.broadcasted_iota(jnp.int32, (512, 40), 0)
    starts = start_ref[0]
    total = jnp.max(starts + rank_ref[0], axis=1, keepdims=True)
    begun = jnp.where(starts <= slot40, 1.0, 0.0) + jnp.where(total <= slot40, 64.0, 0.0)
    owner = jnp.sum(begun, axis=1, keepdims=True).astype(jnp.int32) - 1
    place[...] = owner - 5 * (lane // 16)
    row = lax.broadcasted_iota(jnp.int32, (1024, 128), 0)
    col = lax.broadcasted_iota(jnp.int32, (1024, 128), 1)
    pack[...] = jnp.where(col == (row // 128) * 16 + row % 16, 1.0, 0.0).astype(BF)
    row = lax.broadcasted_iota(jnp.int32, (512, 128), 0)
    col = lax.broadcasted_iota(jnp.int32, (512, 128), 1)
    target = 64 + ((row // 8) % 2) * 32 + (row // 128) * 8 + (row % 8 + 8 - turn) % 8
    for a in range(8):
        hit = (col == target) & ((row // 16) % 8 == a)
        unpack[:, pl.ds(a * 128, 128)] = jnp.where(hit, 1.0, 0.0).astype(BF)
    n = lax.broadcasted_iota(jnp.int32, (256, 256), 0)
    col = lax.broadcasted_iota(jnp.int32, (256, 256), 1)
    for c in range(2):
        source = ((n % 8) * 16 + n // 16) * 2 + c
        pick = jnp.where(col == source, 2.0, 0.0).astype(BF)
        for kk in range(2):
            table[kk * 2 + c] = jnp.dot(pick, f[kk], preferred_element_type=F32).astype(BF)

    meta_all.wait_recv()
    slot = lax.broadcasted_iota(jnp.int32, (512, 128), 0).astype(F32)
    weight = jnp.where(lane == 40, 64.0, 1.0)
    for row in range(4):
        begun = jnp.where(meta[row, 0:1, :] <= slot, weight, 0.0)
        owner = jnp.sum(begun, axis=1, keepdims=True).astype(jnp.int32) - 1
        place4[row] = owner - 5 * (lane // 16)
    for a in (0, 2, 1, 3):
        v_pass(a)
    g_send(0)
    for i in range(3):
        forward(i)
    g_send(1)
    for i in range(3, 16):
        forward(i)
    for i in range(16):
        relay(i)
    for a in range(4):
        v_copy(a, a >= 2).wait_recv()
    v_whole(vs.at[0], v2, None).wait_recv()
    g_all(1).wait_recv()
    own_products()
    for load in loads[2:5]:
        load.wait()
    settle()
    for jj in range(5):
        if jj < 4:
            whole(0, x, xs.at[0], x2.at[jj], 320).wait_recv()
        products(jj)
    e = jnp.dot(u[0].reshape(512, 512), coefficients(), preferred_element_type=F32)
    e = e + jnp.dot(u[1].reshape(512, 512), other_coefficients(), preferred_element_type=F32)
    bb[...] = (e[:256] + swapped(e[256:], 32)).astype(BF)

    def y_back(i):
        d = YSTEPS[i]
        rows = pl.ds(pl.multiple_of(((y + d) % 8) * 32, 32), 32)
        return send(bb.at[rows], ry.at[y], fs.at[0], fs.at[1], y_peer(d))

    def g_back(i):
        d = STEPS[i]
        return send(pz.at[g_to(d)], rz.at[me_g], fs.at[2], fs.at[3], g_peer(d))

    y_back_all = send(ry.at[pl.ds(0, 7)], ry.at[pl.ds(0, 7)], fs.at[0], fs.at[1], y_peer(1))
    g_back_all = send(rz.at[pl.ds(0, 15)], rz.at[pl.ds(0, 15)], fs.at[2], fs.at[3], g_peer(STEPS[0]))

    for i in range(7):
        y_back(i).start()
    ry[y] = bb[pl.ds(pl.multiple_of(y * 32, 32), 32)]
    source = (n % 8) * 32 + (n // 16) * 2 + (n // 8) % 2
    pick = jnp.where(col == source, 1.0, 0.0).astype(BF)
    y_back_all.wait_recv()
    moved = jnp.dot(pick, ry[...].reshape(256, 128), preferred_element_type=F32)
    pz[...] = moved.astype(BF).reshape(16, 16, 128)
    for i in range(15):
        g_back(i).start()
    rz[me_g] = pz[me_g]
    g_back_all.wait_recv()
    turned = jnp.transpose(rz[...].reshape(256, 128).astype(F32))
    lane = lax.broadcasted_iota(jnp.int32, (32, 256), 1)
    series = jnp.zeros((64, 1024), F32)
    for b in range(4):
        part = turned[b * 32 : (b + 1) * 32]
        lhs = jnp.concatenate([jnp.where((lane // 8) % 2 == q, part, 0.0) for q in range(2)], axis=0)
        series = series + jnp.dot(lhs.astype(BF), table[b], preferred_element_type=F32)
    out_ref[...] = series.astype(BF)

    for kk in range(2):
        y_all(kk).wait_send()
        g_all(kk).wait_send()
    for a in range(2):
        whole(0, x, xs.at[a], x2.at[0]).wait_send()
        whole(0, x, xs2.at[a], x2.at[0], 640).wait_send()
        v_whole(vs.at[a], v2, None).wait_send()
        v_whole(vs2.at[a], v2, 0).wait_send()
    meta_all.wait_send()
    coeffs_all.wait_send()
    y_back_all.wait_send()
    g_back_all.wait_send()


VM = pl.BlockSpec(memory_space=pltpu.VMEM)
ANY = pl.BlockSpec(memory_space=pl.ANY)
DMA = pltpu.SemaphoreType.DMA


def per_device(wavefield, u_factors, v_factors, tile_ranks, tile_offsets):
    series = pl.pallas_call(
        kernel,
        out_shape=pltpu.VMEM((64, 1024), BF),
        in_specs=[ANY] * 5,
        out_specs=VM,
        scratch_shapes=[
            pltpu.VMEM((2, 1, 40), jnp.int32),
            pltpu.VMEM((2, 1, 40), jnp.int32),
            pltpu.VMEM((640, 1024), BF),
            pltpu.VMEM((2, 512, 256), BF),
            pltpu.VMEM((4, 2, 512, 256), BF),
            pltpu.VMEM((2, 2, 256, 512), BF),
            pltpu.VMEM((2, 256, 1024), BF),
            pltpu.VMEM((2, 640, 128), F32),
            pltpu.VMEM((2, 8, 80, 256), BF),
            pltpu.VMEM((2, 8, 80, 256), BF),
            pltpu.VMEM((1024, 1024), BF),
            pltpu.VMEM((1024, 128), BF),
            pltpu.VMEM((512, 1024), BF),
            pltpu.VMEM((2, 16, 80, 128), BF),
            pltpu.VMEM((4, 2, 1280, 128), BF),
            pltpu.VMEM((8, 128), F32),
            pltpu.VMEM((4, 8, 128), F32),
            pltpu.VMEM((512, 128), jnp.int32),
            pltpu.VMEM((4, 512, 128), jnp.int32),
            pltpu.VMEM((1024, 512), F32),
            pltpu.VMEM((4, 64, 128), BF),
            pltpu.VMEM((4, 64, 128), BF),
            pltpu.VMEM((4, 256, 1024), BF),
            pltpu.VMEM((256, 128), BF),
            pltpu.VMEM((8, 32, 128), BF),
            pltpu.VMEM((16, 16, 128), BF),
            pltpu.VMEM((16, 16, 128), BF),
            DMA((7,)),
            DMA((2,)),
            DMA((2,)),
            DMA((2,)),
            DMA((16,)),
            DMA((2,)),
            DMA((9,)),
            DMA((9,)),
            DMA((4,)),
            DMA((2,)),
            DMA((4,)),
            DMA((2,)),
            DMA((4,)),
            DMA((4,)),
            DMA,
            DMA((2,)),
            DMA,
            DMA,
            DMA,
            DMA,
        ],
        compiler_params=pltpu.CompilerParams(
            collective_id=0, has_side_effects=True, vmem_limit_bytes=56 * 1024 * 1024
        ),
    )(wavefield.reshape(640, 1024), v_factors[:, :, 0], u_factors[:, :, 0], tile_ranks[:, 0:1], tile_offsets[:, 0:1])
    return series.reshape(2, 32, 1024)


def solution(mesh):
    torus = Mesh(
        mesh.devices.reshape(8, 8, 2, mesh.shape["rows"]), ("freq_0", "freq_1", "freq_2", "rows")
    )
    return jax.shard_map(
        per_device,
        mesh=torus,
        in_specs=(
            P(FREQ, "rows", None),
            P(None, FREQ, "rows", None, None),
            P(None, FREQ, "rows", None, None),
            P(FREQ, "rows", None),
            P(FREQ, "rows", None),
        ),
        out_specs=P(ROWS_FREQ, None, None),
        check_vma=False,
    )
```

```python
import math

import jax
import jax.numpy as jnp
import numpy as np
from jax import lax
from jax.experimental import pallas as pl
from jax.experimental.pallas import tpu as pltpu
from jax.sharding import Mesh
from jax.sharding import PartitionSpec as P

FREQ = ("freq_0", "freq_1", "freq_2")
ROWS_FREQ = ("rows", "freq_0", "freq_1", "freq_2")
BF = jnp.bfloat16
F32 = jnp.float32
MESH = pl.DeviceIdType.MESH

_z = 0.125 * (1.0 - np.cos(np.pi * (np.arange(64) + 0.5) / 64))
COS = [float(a) for a in np.polynomial.polynomial.polyfit(_z, np.cos(2 * np.pi * np.sqrt(_z)), 9)]

STEPS = [(0, 1)] + [(d, c) for d in (1, 7, 4, 5, 3, 2, 6) for c in (0, 1)]
YSTEPS = (4, 3, 5, 2, 6, 1, 7)


def cosine(m):
    x = jnp.where(m >= 512, m - 1024, m).astype(F32) * (1.0 / 1024.0)
    z = x * x
    value = jnp.full(m.shape, COS[-1], F32)
    for a in COS[-2::-1]:
        value = value * z + a
    return value


def build_table(f_ref, kk):
    turn = (((lax.broadcasted_iota(jnp.int32, (8, 128), 0) // 2) * 2 + (kk + 1)) * 128) & 1023
    cos8 = jnp.concatenate([cosine(turn)] * 8, axis=0)
    sin8 = jnp.concatenate([cosine((turn + 768) & 1023)] * 8, axis=0)
    for part in range(4):
        row = lax.broadcasted_iota(jnp.int32, (64, 128), 0) + part * 64
        lane = lax.broadcasted_iota(jnp.int32, (64, 128), 1)
        k1 = (row // 2) * 2 + (kk + 1)
        m = (k1 * lane + (row % 2) * 256) & 1023
        co, si = cosine(m), cosine((m + 768) & 1023)
        ct, st = cos8, sin8
        for b in range(8):
            f_ref[kk, pl.ds(part * 64, 64), pl.ds(b * 128, 128)] = (co * (1.0 / 32.0)).astype(BF)
            if b < 7:
                co, si = co * ct - si * st, si * ct + co * st


def one_hot(shape, source):
    row = lax.broadcasted_iota(jnp.int32, shape, 0)
    return jnp.where(row == source, 1.0, 0.0).astype(BF)


def swapped(b, width):
    lane = lax.broadcasted_iota(jnp.int32, b.shape, 1)
    real = (lane // width) % 2 == 0
    return jnp.where(real, -pltpu.roll(b, b.shape[1] - width, axis=1), pltpu.roll(b, width, axis=1))


def kernel(
    w_hbm, v_hbm, u_hbm, rank_hbm, start_hbm, out_ref,
    rank_ref, start_ref, w, v, vg, u, f, o, s1, r1, perm, pack, unpack, p2, g, mine, meta, place, place4, acc, cs, cr,
    table, bb, ry, pz, rz,
    load_sem, s1s, r1s, p2s, p2r, xs, xm, xp, x2, xs2, fs,
    vs, vm, vp, v2, vs2, ms, mr, css, crs,
):
    y = lax.axis_index("freq_0")
    z = lax.axis_index("freq_1")
    core = lax.axis_index("freq_2")
    x = lax.axis_index("rows")
    me_g = z * 2 + core

    loads = [
        pltpu.make_async_copy(w_hbm, w, load_sem.at[0]),
        pltpu.make_async_copy(v_hbm.at[:, 1], vg.at[x], load_sem.at[1]),
        pltpu.make_async_copy(v_hbm.at[:, 0], v, load_sem.at[2]),
        pltpu.make_async_copy(u_hbm.at[:, 0], u.at[0], load_sem.at[3]),
        pltpu.make_async_copy(u_hbm.at[:, 1], u.at[1], load_sem.at[4]),
        pltpu.make_async_copy(rank_hbm, rank_ref, load_sem.at[5]),
        pltpu.make_async_copy(start_hbm, start_ref, load_sem.at[6]),
    ]
    def y_peer(d):
        return {"freq_0": (y + d) % 8}

    def g_peer(d):
        return {"freq_1": (z + d[0]) % 8, "freq_2": (core + d[1]) % 2}

    def g_to(d):
        return ((z + d[0]) % 8) * 2 + (core + d[1]) % 2

    def g_from(d):
        return ((z + 8 - d[0]) % 8) * 2 + (core + 2 - d[1]) % 2

    x_up, x_down = (x + 1) % 4, (x + 3) % 4

    barrier = pltpu.get_barrier_semaphore()
    loads[0].start()
    for d in sorted(STEPS, key=lambda d: -min(d[0], 8 - d[0])):
        pl.semaphore_signal(barrier, inc=1, device_id=g_peer(d), device_id_type=MESH)
    for d in YSTEPS:
        pl.semaphore_signal(barrier, inc=1, device_id=y_peer(d), device_id_type=MESH)
    for peer in ((x + 2) % 4, x_up, x_down):
        pl.semaphore_signal(barrier, inc=1, device_id={"rows": peer}, device_id_type=MESH)
    for load in loads[1:]:
        load.start()

    def send(src, dst, ssem, rsem, peer):
        return pltpu.make_async_remote_copy(
            src_ref=src, dst_ref=dst, send_sem=ssem, recv_sem=rsem, device_id=peer, device_id_type=MESH
        )

    def y_copy(kk, i):
        d = YSTEPS[i]
        return send(s1.at[kk, (y + d) % 8], r1.at[kk, y], s1s.at[kk], r1s.at[kk], y_peer(d))

    def y_all(kk):
        ref = r1.at[kk, pl.ds(0, 7)]
        return send(ref, ref, s1s.at[kk], r1s.at[kk], y_peer(1))

    def g_copy(kk, i):
        d = STEPS[i]
        rows = pl.ds(me_g * 80, 80)
        return send(p2.at[kk, g_to(d)], g.at[x, kk, rows], p2s.at[kk], p2r.at[15 if kk else i], g_peer(d))

    def g_all(kk):
        ref = g.at[x, kk, pl.ds(0, 1200)]
        return send(ref, ref, p2s.at[kk], p2r.at[15], g_peer(STEPS[0]))

    def block(gs, owner):
        return g.at[owner, 0, pl.ds(gs * 80, 80)]

    def x_copy(gs, up):
        ref = block(gs, x)
        if up:
            return send(ref, ref, xs.at[0], xm.at[8 - (8 - gs // 2) * (1 - gs % 2)], {"rows": x_up})
        return send(ref, ref, xs.at[1], xp.at[8 - (8 - gs // 2) * (gs % 2)], {"rows": x_down})

    def x_relay(gs):
        if gs % 2 == 0:
            ref = block(gs, x_down)
            return send(ref, ref, xs2.at[0], x2.at[gs // 4], {"rows": x_up})
        ref = block(gs, x_up)
        return send(ref, ref, xs2.at[1], x2.at[gs // 4], {"rows": x_down})

    def v_copy(a, up):
        ref = vg.at[x, a // 2, pl.ds((a % 2) * 256, 256)]
        if up:
            return send(ref, ref, vs.at[0], vm.at[a], {"rows": x_up})
        return send(ref, ref, vs.at[1], vp.at[a], {"rows": x_down})

    def v_relay(a):
        rows = pl.ds((a % 2) * 256, 256)
        if a < 2:
            ref = vg.at[x_down, a // 2, rows]
            return send(ref, ref, vs2.at[0], v2, {"rows": x_up})
        ref = vg.at[x_up, a // 2, rows]
        return send(ref, ref, vs2.at[1], v2, {"rows": x_down})

    def v_pass(a):
        v_copy(a, a < 2).wait_recv()
        v_relay(a).start()

    def meta_copy(d):
        return send(mine, meta.at[x], ms, mr, {"rows": (x + d) % 4})

    meta_all = send(meta.at[pl.ds(0, 3)], meta.at[pl.ds(0, 3)], ms, mr, {"rows": x_up})

    def coeff_copy(d):
        return send(cs.at[(x + d) % 4], cr.at[x], css, crs, {"rows": (x + d) % 4})

    coeffs_all = send(cs.at[pl.ds(0, 3)], cr.at[pl.ds(0, 3)], css, crs, {"rows": x_up})

    def v_whole(ssem, rsem, part):
        ref = vg.at[x] if part is None else vg.at[x, part]
        return send(ref, ref, ssem, rsem, {"rows": x_up})

    def dft(kk):
        both = lax.dot_general(w[...], f[kk], (((1,), (1,)), ((), ())), preferred_element_type=F32)
        for half in range(2):
            o[half] = both[:, half * 128 : (half + 1) * 128]
        slot = lax.broadcasted_iota(jnp.int32, (16, 128), 1) // 16
        bits = [(slot // 2**a) % 2 == 1 for a in range(3)]

        def place_rows(chunk, carry):
            for half in range(2):
                value = [None] * 8
                for s in range(8):
                    t = o[half, pl.ds(chunk * 128 + s, 16, stride=8), :]
                    value[(-s) % 8] = pltpu.roll(t, 16 * s, axis=1) if s else t
                for a in range(3):
                    value = [jnp.where(bits[a], value[(b - 2**a) % 8], value[b]) for b in range(8)]
                for b in range(8):
                    rows = pl.ds(pl.multiple_of(chunk * 16, 16), 16)
                    s1[kk, half * 4 + b // 2, rows, pl.ds((b % 2) * 128, 128)] = value[b].astype(BF)
            return carry

        lax.fori_loop(0, 5, place_rows, 0, unroll=True)

    def y_send(kk):
        for i in range(7):
            y_copy(kk, i).start()
        r1[kk, y] = s1[kk, y]

    def g_send(kk):
        y_all(kk).wait_recv()
        lhs = jnp.concatenate(
            [
                jnp.concatenate([r1[kk, a, :, pl.ds(h * 128, 128)] for a in range(8)], axis=1)
                for h in range(2)
            ],
            axis=0,
        )
        for dz in (0, 1, 3, 2):
            b = ((z + dz) % 4) * 2
            cols = pl.ds(pl.multiple_of(b * 128, 256), 256)
            moved = jnp.dot(lhs, perm[:, cols], preferred_element_type=F32).astype(BF)
            for c in range(2):
                p2[kk, b + c] = moved[:80, c * 128 : (c + 1) * 128]
                p2[kk, 8 + b + c] = moved[80:, c * 128 : (c + 1) * 128]
            for d in (dz, dz + 4):
                for dc in (1, 0):
                    if (d, dc) == (0, 0):
                        g[x, kk, pl.ds(pl.multiple_of(me_g * 80, 16), 80)] = p2[kk, me_g]
                    else:
                        g_copy(kk, STEPS.index((d, dc))).start()

    def forward(i):
        gs = me_g
        if i > 0:
            g_copy(0, i - 1).wait_recv()
            gs = g_from(STEPS[i - 1])
        x_copy(gs, True).start()
        x_copy(gs, False).start()

    def relay(gs):
        x_copy(gs, gs % 2 == 0).wait_recv()
        x_relay(gs).start()

    def whole(kk, owner, ssem, rsem, rows=1280):
        ref = g.at[owner, kk, pl.ds(0, rows)]
        return send(ref, ref, ssem, rsem, {"rows": x_up})

    def settle():
        whole(0, x, xs.at[0], xm.at[8], 640).wait_recv()
        whole(0, x, xs.at[0], xp.at[8], 640).wait_recv()

    def products(factors, tiles, kk, source, owner, lanes):
        rhs = jnp.concatenate([g[source, kk, pl.ds(jj * 256, 256), :] for jj in tiles], axis=1)
        prod = jnp.dot(factors, rhs, preferred_element_type=F32)
        for m, jj in enumerate(tiles):
            hit = owner == jj
            for ab in range(2):
                rows = pl.ds(ab * 512, 512)
                old = acc[rows, lanes] if jj else 0.0
                new = prod[ab * 512 : (ab + 1) * 512, m * 128 : (m + 1) * 128]
                acc[rows, lanes] = jnp.where(hit, new, old)

    def combined(lanes):
        return (acc[pl.ds(0, 512), lanes] + swapped(acc[pl.ds(512, 512), lanes], 8)).astype(BF)

    def half_coefficients(d):
        row = lax.broadcasted_iota(jnp.int32, (128, 128), 0)
        col = lax.broadcasted_iota(jnp.int32, (128, 128), 1)
        c, s = (row // 8) % 2, (row % 8 + 8 - turn) % 8
        join = jnp.where(col == c * 32 + ((x + d) % 4) * 8 + s, 1.0, 0.0).astype(BF)
        return jnp.dot(combined(pl.ds(d * 128, 128)), join, preferred_element_type=F32)

    def own_products(steps):
        lhs = []
        for d in steps:
            row = (x + d) % 4
            factors = vg[row].reshape(1024, 256)
            lanes = pl.ds(d * 128, 128)
            for tiles in ((0, 1), (2, 3), (4,)):
                products(factors, tiles, 1, x, place4[row], lanes)
            value = combined(lanes)
            lhs.append(jnp.concatenate([value[a * 64 : (a + 1) * 64] for a in range(8)], axis=1))
        packed = jnp.dot(jnp.concatenate(lhs, axis=0), pack[...], preferred_element_type=F32).astype(BF)
        for m, d in enumerate(steps):
            cs[(x + d) % 4] = packed[m * 64 : (m + 1) * 64]
            if d:
                coeff_copy(d).start()
            else:
                cr[x] = cs[x]

    def other_coefficients():
        coeffs_all.wait_recv()
        lhs = jnp.concatenate([cr[a] for a in range(4)], axis=1)
        wide = jnp.dot(lhs, unpack[...], preferred_element_type=F32).astype(BF)
        return jnp.concatenate([wide[:, a * 128 : (a + 1) * 128] for a in range(8)], axis=0)

    turn = (y % 4) * 2 + z // 4

    build_table(f, 0)
    loads[0].wait()
    dft(0)
    pl.semaphore_wait(barrier, 25)
    y_send(0)
    loads[5].wait()
    loads[6].wait()
    mine[...] = jnp.full((8, 128), 1e9, F32)
    mine[0:1, 0:40] = start_ref[1].astype(F32)
    mine[0:1, 40:41] = jnp.max(start_ref[1] + rank_ref[1], axis=1, keepdims=True).astype(F32)
    for d in range(1, 4):
        meta_copy(d).start()
    meta[x] = mine[...]
    loads[1].wait()
    for a in range(4):
        v_copy(a, True).start()
        v_copy((a + 2) % 4, False).start()
    build_table(f, 1)
    dft(1)
    y_send(1)

    col = lax.broadcasted_iota(jnp.int32, (1024, 128), 1)
    for b in range(8):
        perm[:, pl.ds(b * 128, 128)] = one_hot(
            (1024, 128), (col // 16) * 128 + (col % 8) * 16 + b * 2 + (col // 8) % 2
        )
    lane = lax.broadcasted_iota(jnp.int32, (512, 128), 1)
    slot40 = lax.broadcasted_iota(jnp.int32, (512, 40), 0)
    starts = start_ref[0]
    total = jnp.max(starts + rank_ref[0], axis=1, keepdims=True)
    begun = jnp.where(starts <= slot40, 1.0, 0.0) + jnp.where(total <= slot40, 64.0, 0.0)
    owner = jnp.sum(begun, axis=1, keepdims=True).astype(jnp.int32) - 1
    place[...] = owner - 5 * (lane // 16)
    row = lax.broadcasted_iota(jnp.int32, (1024, 128), 0)
    col = lax.broadcasted_iota(jnp.int32, (1024, 128), 1)
    pack[...] = jnp.where(col == (row // 128) * 16 + row % 16, 1.0, 0.0).astype(BF)
    row = lax.broadcasted_iota(jnp.int32, (512, 128), 0)
    col = lax.broadcasted_iota(jnp.int32, (512, 128), 1)
    target = 64 + ((row // 8) % 2) * 32 + (row // 128) * 8 + (row % 8 + 8 - turn) % 8
    for a in range(8):
        hit = (col == target) & ((row // 16) % 8 == a)
        unpack[:, pl.ds(a * 128, 128)] = jnp.where(hit, 1.0, 0.0).astype(BF)
    n = lax.broadcasted_iota(jnp.int32, (256, 256), 0)
    col = lax.broadcasted_iota(jnp.int32, (256, 256), 1)
    n2 = lax.broadcasted_iota(jnp.int32, (128, 256), 0)
    col2 = lax.broadcasted_iota(jnp.int32, (128, 256), 1)
    for c in range(2):
        source = ((n2 % 8) * 16 + n2 // 8) * 2 + c
        pick = jnp.where(col2 == source, 2.0, 0.0).astype(BF)
        for kk in range(2):
            table[kk * 2 + c] = jnp.dot(pick, f[kk], preferred_element_type=F32).astype(BF)

    meta_all.wait_recv()
    slot = lax.broadcasted_iota(jnp.int32, (512, 128), 0).astype(F32)
    weight = jnp.where(lane == 40, 64.0, 1.0)
    for row in range(4):
        begun = jnp.where(meta[row, 0:1, :] <= slot, weight, 0.0)
        owner = jnp.sum(begun, axis=1, keepdims=True).astype(jnp.int32) - 1
        place4[row] = owner - 5 * (lane // 16)
    for a in (0, 2, 1, 3):
        v_pass(a)
    g_send(0)
    for i in range(3):
        forward(i)
    g_send(1)
    for i in range(3, 16):
        forward(i)
    for i in range(12):
        relay(i)
    for a in range(4):
        v_copy(a, a >= 2).wait_recv()
    v_whole(vs.at[0], v2, None).wait_recv()
    g_all(1).wait_recv()
    own_products((2, 1))
    for i in range(12, 16):
        relay(i)
    own_products((3, 0))
    for load in loads[2:5]:
        load.wait()
    settle()
    factors = v[...].reshape(1024, 256)
    total = jnp.zeros((512, 128), F32)
    for d in (0, 1, 3):
        for tiles in ((0, 1), (2, 3), (4,)):
            products(factors, tiles, 0, (x + d) % 4, place[...], pl.ds(d * 128, 128))
        total = total + half_coefficients(d)
    for groups, tiles in (((0, 1), (0, 1)), ((2,), (2,)), ((3,), (3, 4))):
        if tiles == (3, 4):
            e = jnp.dot(u[1].reshape(512, 512), other_coefficients(), preferred_element_type=F32)
        for a in groups:
            whole(0, x, xs.at[0], x2.at[a], 320).wait_recv()
        products(factors, tiles, 0, (x + 2) % 4, place[...], pl.ds(256, 128))
    total = total + half_coefficients(2)
    e = e + jnp.dot(u[0].reshape(512, 512), total.astype(BF), preferred_element_type=F32)
    bb[...] = (e[:256] + swapped(e[256:], 32)).astype(BF)

    def y_back(i):
        d = YSTEPS[i]
        rows = pl.ds(pl.multiple_of(((y + d) % 8) * 32, 32), 32)
        return send(bb.at[rows], ry.at[y], fs.at[0], fs.at[1], y_peer(d))

    def g_back(i):
        d = STEPS[i]
        return send(pz.at[g_to(d)], rz.at[me_g], fs.at[2], fs.at[3], g_peer(d))

    y_back_all = send(ry.at[pl.ds(0, 7)], ry.at[pl.ds(0, 7)], fs.at[0], fs.at[1], y_peer(1))
    g_back_all = send(rz.at[pl.ds(0, 15)], rz.at[pl.ds(0, 15)], fs.at[2], fs.at[3], g_peer(STEPS[0]))

    for i in range(7):
        y_back(i).start()
    ry[y] = bb[pl.ds(pl.multiple_of(y * 32, 32), 32)]
    source = (n % 8) * 32 + (n // 16) * 2 + (n // 8) % 2
    pick = jnp.where(col == source, 1.0, 0.0).astype(BF)
    y_back_all.wait_recv()
    moved = jnp.dot(pick, ry[...].reshape(256, 128), preferred_element_type=F32)
    pz[...] = moved.astype(BF).reshape(16, 16, 128)
    for i in range(15):
        g_back(i).start()
    rz[me_g] = pz[me_g]
    g_back_all.wait_recv()
    landed = rz[...].astype(F32)
    turned = [jnp.transpose(landed[:, q * 8 : (q + 1) * 8].reshape(128, 128)) for q in range(2)]
    series = jnp.zeros((64, 1024), F32)
    for b in range(4):
        lhs = jnp.concatenate([turned[q][b * 32 : (b + 1) * 32] for q in range(2)], axis=0)
        series = series + jnp.dot(lhs.astype(BF), table[b], preferred_element_type=F32)
    out_ref[...] = series.astype(BF)

    for kk in range(2):
        y_all(kk).wait_send()
        g_all(kk).wait_send()
    for a in range(2):
        whole(0, x, xs.at[a], x2.at[0]).wait_send()
        whole(0, x, xs2.at[a], x2.at[0], 640).wait_send()
        v_whole(vs.at[a], v2, None).wait_send()
        v_whole(vs2.at[a], v2, 0).wait_send()
    meta_all.wait_send()
    coeffs_all.wait_send()
    y_back_all.wait_send()
    g_back_all.wait_send()


VM = pl.BlockSpec(memory_space=pltpu.VMEM)
ANY = pl.BlockSpec(memory_space=pl.ANY)
DMA = pltpu.SemaphoreType.DMA


def per_device(wavefield, u_factors, v_factors, tile_ranks, tile_offsets):
    series = pl.pallas_call(
        kernel,
        out_shape=pltpu.VMEM((64, 1024), BF),
        in_specs=[ANY] * 5,
        out_specs=VM,
        scratch_shapes=[
            pltpu.VMEM((2, 1, 40), jnp.int32),
            pltpu.VMEM((2, 1, 40), jnp.int32),
            pltpu.VMEM((640, 1024), BF),
            pltpu.VMEM((2, 512, 256), BF),
            pltpu.VMEM((4, 2, 512, 256), BF),
            pltpu.VMEM((2, 2, 256, 512), BF),
            pltpu.VMEM((2, 256, 1024), BF),
            pltpu.VMEM((2, 640, 128), F32),
            pltpu.VMEM((2, 8, 80, 256), BF),
            pltpu.VMEM((2, 8, 80, 256), BF),
            pltpu.VMEM((1024, 1024), BF),
            pltpu.VMEM((1024, 128), BF),
            pltpu.VMEM((512, 1024), BF),
            pltpu.VMEM((2, 16, 80, 128), BF),
            pltpu.VMEM((4, 2, 1280, 128), BF),
            pltpu.VMEM((8, 128), F32),
            pltpu.VMEM((4, 8, 128), F32),
            pltpu.VMEM((512, 128), jnp.int32),
            pltpu.VMEM((4, 512, 128), jnp.int32),
            pltpu.VMEM((1024, 512), F32),
            pltpu.VMEM((4, 64, 128), BF),
            pltpu.VMEM((4, 64, 128), BF),
            pltpu.VMEM((4, 128, 1024), BF),
            pltpu.VMEM((256, 128), BF),
            pltpu.VMEM((8, 32, 128), BF),
            pltpu.VMEM((16, 16, 128), BF),
            pltpu.VMEM((16, 16, 128), BF),
            DMA((7,)),
            DMA((2,)),
            DMA((2,)),
            DMA((2,)),
            DMA((16,)),
            DMA((2,)),
            DMA((9,)),
            DMA((9,)),
            DMA((4,)),
            DMA((2,)),
            DMA((4,)),
            DMA((2,)),
            DMA((4,)),
            DMA((4,)),
            DMA,
            DMA((2,)),
            DMA,
            DMA,
            DMA,
            DMA,
        ],
        compiler_params=pltpu.CompilerParams(
            collective_id=0, has_side_effects=True, vmem_limit_bytes=56 * 1024 * 1024
        ),
    )(wavefield.reshape(640, 1024), v_factors[:, :, 0], u_factors[:, :, 0], tile_ranks[:, 0:1], tile_offsets[:, 0:1])
    return series.reshape(2, 32, 1024)


def solution(mesh):
    torus = Mesh(
        mesh.devices.reshape(8, 8, 2, mesh.shape["rows"]), ("freq_0", "freq_1", "freq_2", "rows")
    )
    return jax.shard_map(
        per_device,
        mesh=torus,
        in_specs=(
            P(FREQ, "rows", None),
            P(None, FREQ, "rows", None, None),
            P(None, FREQ, "rows", None, None),
            P(FREQ, "rows", None),
            P(FREQ, "rows", None),
        ),
        out_specs=P(ROWS_FREQ, None, None),
        check_vma=False,
    )
```

```python
import math

import jax
import jax.numpy as jnp
import numpy as np
from jax import lax
from jax.experimental import pallas as pl
from jax.experimental.pallas import tpu as pltpu
from jax.sharding import Mesh
from jax.sharding import PartitionSpec as P

FREQ = ("freq_0", "freq_1", "freq_2")
ROWS_FREQ = ("rows", "freq_0", "freq_1", "freq_2")
BF = jnp.bfloat16
F32 = jnp.float32
MESH = pl.DeviceIdType.MESH

_z = 0.125 * (1.0 - np.cos(np.pi * (np.arange(64) + 0.5) / 64))
COS = [float(a) for a in np.polynomial.polynomial.polyfit(_z, np.cos(2 * np.pi * np.sqrt(_z)), 9)]

STEPS = [(0, 1)] + [(d, c) for d in (1, 7, 4, 5, 3, 2, 6) for c in (0, 1)]
YSTEPS = (4, 3, 5, 2, 6, 1, 7)


def cosine(m):
    x = jnp.where(m >= 512, m - 1024, m).astype(F32) * (1.0 / 1024.0)
    z = x * x
    value = jnp.full(m.shape, COS[-1], F32)
    for a in COS[-2::-1]:
        value = value * z + a
    return value


def build_table(f_ref, kk):
    turn = (((lax.broadcasted_iota(jnp.int32, (8, 128), 0) // 2) * 2 + (kk + 1)) * 128) & 1023
    cos8 = jnp.concatenate([cosine(turn)] * 8, axis=0)
    sin8 = jnp.concatenate([cosine((turn + 768) & 1023)] * 8, axis=0)
    for part in range(4):
        row = lax.broadcasted_iota(jnp.int32, (64, 128), 0) + part * 64
        lane = lax.broadcasted_iota(jnp.int32, (64, 128), 1)
        k1 = (row // 2) * 2 + (kk + 1)
        m = (k1 * lane + (row % 2) * 256) & 1023
        co, si = cosine(m), cosine((m + 768) & 1023)
        ct, st = cos8, sin8
        for b in range(8):
            f_ref[kk, pl.ds(part * 64, 64), pl.ds(b * 128, 128)] = (co * (1.0 / 32.0)).astype(BF)
            if b < 7:
                co, si = co * ct - si * st, si * ct + co * st


def one_hot(shape, source):
    row = lax.broadcasted_iota(jnp.int32, shape, 0)
    return jnp.where(row == source, 1.0, 0.0).astype(BF)


def swapped(b, width):
    lane = lax.broadcasted_iota(jnp.int32, b.shape, 1)
    real = (lane // width) % 2 == 0
    return jnp.where(real, -pltpu.roll(b, b.shape[1] - width, axis=1), pltpu.roll(b, width, axis=1))


def kernel(
    w_hbm, v_hbm, u_hbm, rank_hbm, start_hbm, out_ref,
    rank_ref, start_ref, w, v, vg, u, f, o, s1, r1, perm, pack, unpack, p2, g, mine, meta, place, place4, acc, cs, cr,
    table, bb, ry, pz, rz,
    load_sem, s1s, r1s, p2s, p2r, xs, xm, xp, x2, xs2, fs,
    vs, vm, vp, v2, vs2, ms, mr, css, crs,
):
    y = lax.axis_index("freq_0")
    z = lax.axis_index("freq_1")
    core = lax.axis_index("freq_2")
    x = lax.axis_index("rows")
    me_g = z * 2 + core

    loads = [
        pltpu.make_async_copy(w_hbm, w, load_sem.at[0]),
        pltpu.make_async_copy(v_hbm.at[:, 1], vg.at[x], load_sem.at[1]),
        pltpu.make_async_copy(v_hbm.at[:, 0], v, load_sem.at[2]),
        pltpu.make_async_copy(u_hbm.at[:, 0], u.at[0], load_sem.at[3]),
        pltpu.make_async_copy(u_hbm.at[:, 1], u.at[1], load_sem.at[4]),
        pltpu.make_async_copy(rank_hbm, rank_ref, load_sem.at[5]),
        pltpu.make_async_copy(start_hbm, start_ref, load_sem.at[6]),
    ]
    def y_peer(d):
        return {"freq_0": (y + d) % 8}

    def g_peer(d):
        return {"freq_1": (z + d[0]) % 8, "freq_2": (core + d[1]) % 2}

    def g_to(d):
        return ((z + d[0]) % 8) * 2 + (core + d[1]) % 2

    def g_from(d):
        return ((z + 8 - d[0]) % 8) * 2 + (core + 2 - d[1]) % 2

    x_up, x_down = (x + 1) % 4, (x + 3) % 4

    barrier = pltpu.get_barrier_semaphore()
    loads[0].start()
    for d in sorted(STEPS, key=lambda d: -min(d[0], 8 - d[0])):
        pl.semaphore_signal(barrier, inc=1, device_id=g_peer(d), device_id_type=MESH)
    for d in YSTEPS:
        pl.semaphore_signal(barrier, inc=1, device_id=y_peer(d), device_id_type=MESH)
    for peer in ((x + 2) % 4, x_up, x_down):
        pl.semaphore_signal(barrier, inc=1, device_id={"rows": peer}, device_id_type=MESH)
    for load in loads[1:]:
        load.start()

    def send(src, dst, ssem, rsem, peer):
        return pltpu.make_async_remote_copy(
            src_ref=src, dst_ref=dst, send_sem=ssem, recv_sem=rsem, device_id=peer, device_id_type=MESH
        )

    def y_copy(kk, i):
        d = YSTEPS[i]
        return send(s1.at[kk, (y + d) % 8], r1.at[kk, y], s1s.at[kk], r1s.at[kk], y_peer(d))

    def y_all(kk):
        ref = r1.at[kk, pl.ds(0, 7)]
        return send(ref, ref, s1s.at[kk], r1s.at[kk], y_peer(1))

    def g_copy(kk, i):
        d = STEPS[i]
        rows = pl.ds(me_g * 80, 80)
        return send(p2.at[kk, g_to(d)], g.at[x, kk, rows], p2s.at[kk], p2r.at[15 if kk else i], g_peer(d))

    def g_all(kk):
        ref = g.at[x, kk, pl.ds(0, 1200)]
        return send(ref, ref, p2s.at[kk], p2r.at[15], g_peer(STEPS[0]))

    def block(gs, owner):
        return g.at[owner, 0, pl.ds(gs * 80, 80)]

    def x_copy(gs, up):
        ref = block(gs, x)
        if up:
            return send(ref, ref, xs.at[0], xm.at[8 - (8 - gs // 2) * (1 - gs % 2)], {"rows": x_up})
        return send(ref, ref, xs.at[1], xp.at[8 - (8 - gs // 2) * (gs % 2)], {"rows": x_down})

    def x_relay(gs):
        if gs % 2 == 0:
            ref = block(gs, x_down)
            return send(ref, ref, xs2.at[0], x2.at[gs // 4], {"rows": x_up})
        ref = block(gs, x_up)
        return send(ref, ref, xs2.at[1], x2.at[gs // 4], {"rows": x_down})

    def v_copy(a, up):
        ref = vg.at[x, a // 2, pl.ds((a % 2) * 256, 256)]
        if up:
            return send(ref, ref, vs.at[0], vm.at[a], {"rows": x_up})
        return send(ref, ref, vs.at[1], vp.at[a], {"rows": x_down})

    def v_relay(a):
        rows = pl.ds((a % 2) * 256, 256)
        if a < 2:
            ref = vg.at[x_down, a // 2, rows]
            return send(ref, ref, vs2.at[0], v2, {"rows": x_up})
        ref = vg.at[x_up, a // 2, rows]
        return send(ref, ref, vs2.at[1], v2, {"rows": x_down})

    def v_pass(a):
        v_copy(a, a < 2).wait_recv()
        v_relay(a).start()

    def meta_copy(d):
        return send(mine, meta.at[x], ms, mr, {"rows": (x + d) % 4})

    meta_all = send(meta.at[pl.ds(0, 3)], meta.at[pl.ds(0, 3)], ms, mr, {"rows": x_up})

    def coeff_copy(d):
        return send(cs.at[(x + d) % 4], cr.at[x], css, crs, {"rows": (x + d) % 4})

    coeffs_all = send(cs.at[pl.ds(0, 3)], cr.at[pl.ds(0, 3)], css, crs, {"rows": x_up})

    def v_whole(ssem, rsem, part):
        ref = vg.at[x] if part is None else vg.at[x, part]
        return send(ref, ref, ssem, rsem, {"rows": x_up})

    def dft(kk):
        both = lax.dot_general(w[...], f[kk], (((1,), (1,)), ((), ())), preferred_element_type=F32)
        for half in range(2):
            o[half] = both[:, half * 128 : (half + 1) * 128]
        slot = lax.broadcasted_iota(jnp.int32, (16, 128), 1) // 16
        bits = [(slot // 2**a) % 2 == 1 for a in range(3)]

        def place_rows(chunk, carry):
            for half in range(2):
                value = [None] * 8
                for s in range(8):
                    t = o[half, pl.ds(chunk * 128 + s, 16, stride=8), :]
                    value[(-s) % 8] = pltpu.roll(t, 16 * s, axis=1) if s else t
                for a in range(3):
                    value = [jnp.where(bits[a], value[(b - 2**a) % 8], value[b]) for b in range(8)]
                for b in range(8):
                    rows = pl.ds(pl.multiple_of(chunk * 16, 16), 16)
                    s1[kk, half * 4 + b // 2, rows, pl.ds((b % 2) * 128, 128)] = value[b].astype(BF)
            return carry

        lax.fori_loop(0, 5, place_rows, 0, unroll=True)

    def y_send(kk):
        for i in range(7):
            y_copy(kk, i).start()
        r1[kk, y] = s1[kk, y]

    def g_send(kk):
        y_all(kk).wait_recv()
        lhs = jnp.concatenate(
            [
                jnp.concatenate([r1[kk, a, :, pl.ds(h * 128, 128)] for a in range(8)], axis=1)
                for h in range(2)
            ],
            axis=0,
        )
        for dz in (0, 1, 3, 2):
            b = ((z + dz) % 4) * 2
            cols = pl.ds(pl.multiple_of(b * 128, 256), 256)
            moved = jnp.dot(lhs, perm[:, cols], preferred_element_type=F32).astype(BF)
            for c in range(2):
                p2[kk, b + c] = moved[:80, c * 128 : (c + 1) * 128]
                p2[kk, 8 + b + c] = moved[80:, c * 128 : (c + 1) * 128]
            for d in (dz, dz + 4):
                for dc in (1, 0):
                    if (d, dc) == (0, 0):
                        g[x, kk, pl.ds(pl.multiple_of(me_g * 80, 16), 80)] = p2[kk, me_g]
                    else:
                        g_copy(kk, STEPS.index((d, dc))).start()

    def forward(i):
        gs = me_g
        if i > 0:
            g_copy(0, i - 1).wait_recv()
            gs = g_from(STEPS[i - 1])
        x_copy(gs, True).start()
        x_copy(gs, False).start()

    def relay(gs):
        x_copy(gs, gs % 2 == 0).wait_recv()
        x_relay(gs).start()

    def whole(kk, owner, ssem, rsem, rows=1280):
        ref = g.at[owner, kk, pl.ds(0, rows)]
        return send(ref, ref, ssem, rsem, {"rows": x_up})

    def settle():
        whole(0, x, xs.at[0], xm.at[8], 640).wait_recv()
        whole(0, x, xs.at[0], xp.at[8], 640).wait_recv()

    def products(factors, tiles, kk, source, owner, lanes):
        rhs = jnp.concatenate([g[source, kk, pl.ds(jj * 256, 256), :] for jj in tiles], axis=1)
        prod = jnp.dot(factors, rhs, preferred_element_type=F32)
        for m, jj in enumerate(tiles):
            hit = owner == jj
            for ab in range(2):
                rows = pl.ds(ab * 512, 512)
                old = acc[rows, lanes] if jj else 0.0
                new = prod[ab * 512 : (ab + 1) * 512, m * 128 : (m + 1) * 128]
                acc[rows, lanes] = jnp.where(hit, new, old)

    def combined(lanes):
        return (acc[pl.ds(0, 512), lanes] + swapped(acc[pl.ds(512, 512), lanes], 8)).astype(BF)

    def half_coefficients(d):
        row = lax.broadcasted_iota(jnp.int32, (128, 128), 0)
        col = lax.broadcasted_iota(jnp.int32, (128, 128), 1)
        c, s = (row // 8) % 2, (row % 8 + 8 - turn) % 8
        join = jnp.where(col == c * 32 + ((x + d) % 4) * 8 + s, 1.0, 0.0).astype(BF)
        return jnp.dot(combined(pl.ds(d * 128, 128)), join, preferred_element_type=F32)

    def own_products(steps):
        lhs = []
        for d in steps:
            row = (x + d) % 4
            factors = vg[row].reshape(1024, 256)
            lanes = pl.ds(d * 128, 128)
            for tiles in ((0, 1), (2, 3), (4,)):
                products(factors, tiles, 1, x, place4[row], lanes)
            value = combined(lanes)
            lhs.append(jnp.concatenate([value[a * 64 : (a + 1) * 64] for a in range(8)], axis=1))
        packed = jnp.dot(jnp.concatenate(lhs, axis=0), pack[...], preferred_element_type=F32).astype(BF)
        for m, d in enumerate(steps):
            cs[(x + d) % 4] = packed[m * 64 : (m + 1) * 64]
            if d:
                coeff_copy(d).start()
            else:
                cr[x] = cs[x]

    def other_coefficients():
        coeffs_all.wait_recv()
        lhs = jnp.concatenate([cr[a] for a in range(4)], axis=1)
        wide = jnp.dot(lhs, unpack[...], preferred_element_type=F32).astype(BF)
        return jnp.concatenate([wide[:, a * 128 : (a + 1) * 128] for a in range(8)], axis=0)

    turn = (y % 4) * 2 + z // 4

    build_table(f, 0)
    loads[0].wait()
    dft(0)
    pl.semaphore_wait(barrier, 25)
    y_send(0)
    loads[5].wait()
    loads[6].wait()
    mine[...] = jnp.full((8, 128), 1e9, F32)
    mine[0:1, 0:40] = start_ref[1].astype(F32)
    mine[0:1, 40:41] = jnp.max(start_ref[1] + rank_ref[1], axis=1, keepdims=True).astype(F32)
    for d in range(1, 4):
        meta_copy(d).start()
    meta[x] = mine[...]
    loads[1].wait()
    for a in range(4):
        v_copy(a, True).start()
        v_copy((a + 2) % 4, False).start()
    build_table(f, 1)
    dft(1)
    y_send(1)

    col = lax.broadcasted_iota(jnp.int32, (1024, 128), 1)
    for b in range(8):
        perm[:, pl.ds(b * 128, 128)] = one_hot(
            (1024, 128), (col // 16) * 128 + (col % 8) * 16 + b * 2 + (col // 8) % 2
        )
    lane = lax.broadcasted_iota(jnp.int32, (512, 128), 1)
    slot40 = lax.broadcasted_iota(jnp.int32, (512, 40), 0)
    starts = start_ref[0]
    total = jnp.max(starts + rank_ref[0], axis=1, keepdims=True)
    begun = jnp.where(starts <= slot40, 1.0, 0.0) + jnp.where(total <= slot40, 64.0, 0.0)
    owner = jnp.sum(begun, axis=1, keepdims=True).astype(jnp.int32) - 1
    place[...] = owner - 5 * (lane // 16)
    row = lax.broadcasted_iota(jnp.int32, (1024, 128), 0)
    col = lax.broadcasted_iota(jnp.int32, (1024, 128), 1)
    pack[...] = jnp.where(col == (row // 128) * 16 + row % 16, 1.0, 0.0).astype(BF)
    row = lax.broadcasted_iota(jnp.int32, (512, 128), 0)
    col = lax.broadcasted_iota(jnp.int32, (512, 128), 1)
    target = 64 + ((row // 8) % 2) * 32 + (row // 128) * 8 + (row % 8 + 8 - turn) % 8
    for a in range(8):
        hit = (col == target) & ((row // 16) % 8 == a)
        unpack[:, pl.ds(a * 128, 128)] = jnp.where(hit, 1.0, 0.0).astype(BF)
    n = lax.broadcasted_iota(jnp.int32, (256, 256), 0)
    col = lax.broadcasted_iota(jnp.int32, (256, 256), 1)
    n2 = lax.broadcasted_iota(jnp.int32, (128, 256), 0)
    col2 = lax.broadcasted_iota(jnp.int32, (128, 256), 1)
    for c in range(2):
        source = ((n2 % 8) * 16 + n2 // 8) * 2 + c
        pick = jnp.where(col2 == source, 2.0, 0.0).astype(BF)
        for kk in range(2):
            table[kk * 2 + c] = jnp.dot(pick, f[kk], preferred_element_type=F32).astype(BF)

    meta_all.wait_recv()
    slot = lax.broadcasted_iota(jnp.int32, (512, 128), 0).astype(F32)
    weight = jnp.where(lane == 40, 64.0, 1.0)
    for row in range(4):
        begun = jnp.where(meta[row, 0:1, :] <= slot, weight, 0.0)
        owner = jnp.sum(begun, axis=1, keepdims=True).astype(jnp.int32) - 1
        place4[row] = owner - 5 * (lane // 16)
    for a in (0, 2, 1, 3):
        v_pass(a)
    g_send(0)
    for i in range(3):
        forward(i)
    g_send(1)
    for i in range(3, 16):
        forward(i)
    for load in loads[2:5]:
        load.wait()
    factors = v[...].reshape(1024, 256)

    def source_block(d):
        for tiles in ((0, 1), (2, 3), (4,)):
            products(factors, tiles, 0, (x + d) % 4, place[...], pl.ds(d * 128, 128))
        return half_coefficients(d)

    total = source_block(0)
    for i in range(14):
        relay(i)
    for a in range(4):
        v_copy(a, a >= 2).wait_recv()
    v_whole(vs.at[0], v2, None).wait_recv()
    g_all(1).wait_recv()
    own_products((2, 1))
    for i in range(14, 16):
        relay(i)
    own_products((3, 0))
    settle()
    for d in (1, 3):
        total = total + source_block(d)
    for groups, tiles in (((0, 1), (0, 1)), ((2,), (2,)), ((3,), (3, 4))):
        for a in groups:
            whole(0, x, xs.at[0], x2.at[a], 320).wait_recv()
        products(factors, tiles, 0, (x + 2) % 4, place[...], pl.ds(256, 128))
    total = total + half_coefficients(2)
    e = jnp.dot(u[0].reshape(512, 512), total.astype(BF), preferred_element_type=F32)
    e = e + jnp.dot(u[1].reshape(512, 512), other_coefficients(), preferred_element_type=F32)
    bb[...] = (e[:256] + swapped(e[256:], 32)).astype(BF)

    def y_back(i):
        d = YSTEPS[i]
        rows = pl.ds(pl.multiple_of(((y + d) % 8) * 32, 32), 32)
        return send(bb.at[rows], ry.at[y], fs.at[0], fs.at[1], y_peer(d))

    def g_back(i):
        d = STEPS[i]
        return send(pz.at[g_to(d)], rz.at[me_g], fs.at[2], fs.at[3], g_peer(d))

    y_back_all = send(ry.at[pl.ds(0, 7)], ry.at[pl.ds(0, 7)], fs.at[0], fs.at[1], y_peer(1))
    g_back_all = send(rz.at[pl.ds(0, 15)], rz.at[pl.ds(0, 15)], fs.at[2], fs.at[3], g_peer(STEPS[0]))

    for i in range(7):
        y_back(i).start()
    ry[y] = bb[pl.ds(pl.multiple_of(y * 32, 32), 32)]
    source = (n % 8) * 32 + (n // 16) * 2 + (n // 8) % 2
    pick = jnp.where(col == source, 1.0, 0.0).astype(BF)
    y_back_all.wait_recv()
    moved = jnp.dot(pick, ry[...].reshape(256, 128), preferred_element_type=F32)
    pz[...] = moved.astype(BF).reshape(16, 16, 128)
    for i in sorted(range(15), key=lambda i: -min(STEPS[i][0], 8 - STEPS[i][0])):
        g_back(i).start()
    rz[me_g] = pz[me_g]
    g_back_all.wait_recv()
    landed = rz[...].astype(F32)
    turned = [jnp.transpose(landed[:, q * 8 : (q + 1) * 8].reshape(128, 128)) for q in range(2)]
    series = jnp.zeros((64, 1024), F32)
    for b in range(4):
        lhs = jnp.concatenate([turned[q][b * 32 : (b + 1) * 32] for q in range(2)], axis=0)
        series = series + jnp.dot(lhs.astype(BF), table[b], preferred_element_type=F32)
    out_ref[...] = series.astype(BF)

    for kk in range(2):
        y_all(kk).wait_send()
        g_all(kk).wait_send()
    for a in range(2):
        whole(0, x, xs.at[a], x2.at[0]).wait_send()
        whole(0, x, xs2.at[a], x2.at[0], 640).wait_send()
        v_whole(vs.at[a], v2, None).wait_send()
        v_whole(vs2.at[a], v2, 0).wait_send()
    meta_all.wait_send()
    coeffs_all.wait_send()
    y_back_all.wait_send()
    g_back_all.wait_send()


VM = pl.BlockSpec(memory_space=pltpu.VMEM)
ANY = pl.BlockSpec(memory_space=pl.ANY)
DMA = pltpu.SemaphoreType.DMA


def per_device(wavefield, u_factors, v_factors, tile_ranks, tile_offsets):
    series = pl.pallas_call(
        kernel,
        out_shape=pltpu.VMEM((64, 1024), BF),
        in_specs=[ANY] * 5,
        out_specs=VM,
        scratch_shapes=[
            pltpu.VMEM((2, 1, 40), jnp.int32),
            pltpu.VMEM((2, 1, 40), jnp.int32),
            pltpu.VMEM((640, 1024), BF),
            pltpu.VMEM((2, 512, 256), BF),
            pltpu.VMEM((4, 2, 512, 256), BF),
            pltpu.VMEM((2, 2, 256, 512), BF),
            pltpu.VMEM((2, 256, 1024), BF),
            pltpu.VMEM((2, 640, 128), F32),
            pltpu.VMEM((2, 8, 80, 256), BF),
            pltpu.VMEM((2, 8, 80, 256), BF),
            pltpu.VMEM((1024, 1024), BF),
            pltpu.VMEM((1024, 128), BF),
            pltpu.VMEM((512, 1024), BF),
            pltpu.VMEM((2, 16, 80, 128), BF),
            pltpu.VMEM((4, 2, 1280, 128), BF),
            pltpu.VMEM((8, 128), F32),
            pltpu.VMEM((4, 8, 128), F32),
            pltpu.VMEM((512, 128), jnp.int32),
            pltpu.VMEM((4, 512, 128), jnp.int32),
            pltpu.VMEM((1024, 512), F32),
            pltpu.VMEM((4, 64, 128), BF),
            pltpu.VMEM((4, 64, 128), BF),
            pltpu.VMEM((4, 128, 1024), BF),
            pltpu.VMEM((256, 128), BF),
            pltpu.VMEM((8, 32, 128), BF),
            pltpu.VMEM((16, 16, 128), BF),
            pltpu.VMEM((16, 16, 128), BF),
            DMA((7,)),
            DMA((2,)),
            DMA((2,)),
            DMA((2,)),
            DMA((16,)),
            DMA((2,)),
            DMA((9,)),
            DMA((9,)),
            DMA((4,)),
            DMA((2,)),
            DMA((4,)),
            DMA((2,)),
            DMA((4,)),
            DMA((4,)),
            DMA,
            DMA((2,)),
            DMA,
            DMA,
            DMA,
            DMA,
        ],
        compiler_params=pltpu.CompilerParams(
            collective_id=0, has_side_effects=True, vmem_limit_bytes=56 * 1024 * 1024
        ),
    )(wavefield.reshape(640, 1024), v_factors[:, :, 0], u_factors[:, :, 0], tile_ranks[:, 0:1], tile_offsets[:, 0:1])
    return series.reshape(2, 32, 1024)


def solution(mesh):
    torus = Mesh(
        mesh.devices.reshape(8, 8, 2, mesh.shape["rows"]), ("freq_0", "freq_1", "freq_2", "rows")
    )
    return jax.shard_map(
        per_device,
        mesh=torus,
        in_specs=(
            P(FREQ, "rows", None),
            P(None, FREQ, "rows", None, None),
            P(None, FREQ, "rows", None, None),
            P(FREQ, "rows", None),
            P(FREQ, "rows", None),
        ),
        out_specs=P(ROWS_FREQ, None, None),
        check_vma=False,
    )
```
